128 devices in a mesh: row: 8 (over x, core), col: 16 (over z, y).
Axes of the slice: x: 4, y: 4, z: 4, core: 2. Of those that a mesh axis runs over, the one named last changes fastest.
Arguments:
- matrix: float32 [8192, 8192], P('row', 'col'), as said below
- start_vectors: float32 [8192, 512], P(('col', 'row')), may hold values from -6 to 6
- interval: float32 [2], replicated, as said below
Outputs:
- ortho_basis: float32 [8192, 512], P(('col', 'row'))
- projected: float32 [512, 512], replicated
- residual: float32 [8192, 512], P(('col', 'row'))
The draws below stay inside these ranges and needn't reach their ends.
Inputs may be any that keep to these rules, and one draw needn't show every extreme that they name: matrix is exactly symmetric (entry (r, c) equals entry (c, r)); its eigenvalues lie within about -1.45 to 1.45. interval[0] lies in [-1.2, -0.7] and interval[1] in [1.45, 1.9].
All inputs are finite; a program needn't handle non-finite values.
Results may differ from the reference program's by a relative error of at most 0.0003.
Values sent between devices are 32-bit elements.
A program may use at most 128 MiB of HBM per device.

```python
import math
import jax
import jax.numpy as jnp
from jax import lax

K = 512
FILTER_DEG = 3
OUTER = 2
N = 8192


def draw_matrix(key, part):
    entries = jax.random.normal(key, (N, N), jnp.float32)
    return ((entries + entries.T) * (0.5 / math.sqrt(N))).astype(jnp.float32)


def draw_interval(key, part):
    low_key = jax.random.fold_in(key, 11)
    high_key = jax.random.fold_in(key, 23)
    low_end = jax.random.uniform(low_key, (), jnp.float32, -1.2, -0.7)
    high_end = jax.random.uniform(high_key, (), jnp.float32, 1.45, 1.9)
    return jnp.stack([low_end, high_end]).astype(jnp.float32)


def shard_levels(rng, extent, split, least, high):
    def one(axis_at, blocks):
        steps = jax.random.uniform(jax.random.fold_in(jax.random.fold_in(rng, 6), axis_at), (blocks,), jnp.float32, least / len(split), high / len(split))
        return jnp.repeat(jnp.exp(steps), extent[axis_at] // blocks).reshape((-1,) + (1,) * (len(extent) - axis_at - 1))

    gain = one(*split[0])
    for cut in split[1:]:
        gain = gain * one(*cut)
    return gain


def gaussian(rng, extent, deviation, limit, cuts=(), kind=jnp.bfloat16):
    values = jax.random.normal(rng, extent, jnp.float32) * deviation
    if len(cuts) > 0:
        values = shard_levels(rng, extent, cuts, -0.22, 0.18) * values
    return jnp.clip(values, min=-limit, max=limit).astype(kind)


def setup_inputs(seed: int = 0) -> dict:
    keys = jax.random.split(jax.random.key(seed), 4)
    matrix = draw_matrix(jax.random.fold_in(keys[3], 71), 0)
    start_vectors = gaussian(keys[1], (N, K), 1.0, 6.0, ((0, 128),), jnp.float32)
    interval = draw_interval(jax.random.fold_in(keys[3], 71), 0)
    return dict(matrix=matrix, start_vectors=start_vectors, interval=interval)


def product(left, right):
    return jnp.dot(left, right, precision=lax.Precision.HIGHEST, preferred_element_type=jnp.float32)


def tri_solve(factor, values):
    return jax.scipy.linalg.solve_triangular(factor, values, lower=True)


def reference(matrix, start_vectors, interval):
    center = 0.5 * (interval[0] + interval[1])
    half_width = 0.5 * (interval[1] - interval[0])
    total_rows = matrix.shape[0]
    positions = lax.iota(jnp.int32, total_rows)
    diagonal = positions[:, None] == positions[None, :]
    operator = jnp.where(diagonal, matrix - center, matrix) / half_width
    current_start = start_vectors
    for sweep_index in range(OUTER):
        previous = current_start
        current = product(operator, current_start)
        for degree in range(2, FILTER_DEG + 1):
            previous, current = current, 2.0 * product(operator, current) - previous
        mapped = product(operator, current)
        gram_matrix = product(current.T, current) / total_rows
        cross_terms = product(current.T, mapped) / total_rows
        factor = jnp.linalg.cholesky(gram_matrix)
        ortho_basis = tri_solve(factor, current.T).T
        partial_value = tri_solve(factor, cross_terms)
        projected = tri_solve(factor, partial_value.T).T
        current_start = ortho_basis
    residual = tri_solve(factor, mapped.T).T - product(ortho_basis, projected)
    return ortho_basis, projected, residual
```

```python
import jax
import jax.numpy as jnp
from jax import lax
from jax.experimental import pallas as pl
from jax.experimental.pallas import tpu as pltpu
from jax.sharding import Mesh
from jax.sharding import PartitionSpec as P

ROW = ("row_0", "row_1")
COL = ("col_0", "col_1")
ROW_COL = ("row_0", "row_1", "col_0", "col_1")
COL_ROW = ("col_0", "col_1", "row_0", "row_1")
MESH = pl.DeviceIdType.MESH
F32 = jnp.float32
BF16 = jnp.bfloat16
VMEM_LIMIT = 62 * 1024 * 1024
LINKS = ("ya", "yb", "za", "zb"), ("yb", "ya", "zb", "za"), ("za", "zb", "ya", "yb"), ("zb", "za", "yb", "ya")


class Place:
    def __init__(self):
        self.x = lax.axis_index("row_0")
        self.core = lax.axis_index("row_1")
        self.z = lax.axis_index("col_0")
        self.y = lax.axis_index("col_1")
        self.at = {"x": self.x, "y": self.y, "z": self.z}

    def device(self, x=None, core=None, z=None, y=None):
        pick = lambda given, own: own if given is None else given
        return (pick(x, self.x), pick(core, self.core), pick(z, self.z), pick(y, self.y))

    def sibling(self):
        return self.device(core=1 - self.core)

    def partner(self, link):
        v = self.at[link[0]]
        w = v + 1 - 2 * (v % 2) if link[1] == "a" else 3 - v
        return self.device(**{link[0]: w})

    def bit(self, link):
        v = self.at[link[0]]
        return ((v + 1) // 2) % 2 if link[1] == "a" else v // 2


def remote(src, dst, send, recv, device):
    return pltpu.make_async_remote_copy(
        src_ref=src, dst_ref=dst, send_sem=send, recv_sem=recv, device_id=device, device_id_type=MESH
    )


def rows_at(start, size):
    return pl.ds(pl.multiple_of(start, size), size)


def halves(value):
    hi = value.astype(BF16)
    return hi, (value - hi.astype(F32)).astype(BF16)


def dot(left, right):
    return jnp.dot(left, right, preferred_element_type=F32)


def chain_kernel(
    interval, matrix, slab, y3_out, v3_out, z2_out,
    other, m_hi, m_lo, t_hi, t_lo, cols, rows, part, split_c, split_r,
    r1, h1, r2, h2, r3, h3, r4, share,
    tb, rb1, tb2, rb2, own3, got3,
    f_send, f_recv, b_send, b_recv, g_send, g_recv, m_send, m_recv, p_send, p_recv, s_send, s_recv,
):
    me = Place()
    block = me.z * 4 + me.y

    swap = remote(matrix, other, m_send, m_recv, me.sibling())
    swap.start()

    def slab_rows(x, core):
        return rows_at((x * 2 + core) * 64, 64)

    gathers = []
    for d in range(1, 8):
        to_x, to_core = (me.x + d // 2) % 4, (me.core + d) % 2
        for c in range(2):
            copy = remote(
                slab.at[2 * to_core + c], cols.at[0, c, slab_rows(me.x, me.core)],
                g_send.at[d, c], g_recv.at[d, c], me.device(x=to_x, core=to_core),
            )
            copy.start()
            gathers.append((d, c, copy))
    for c in range(2):
        cols[0, c, slab_rows(me.x, me.core), :] = slab[2 * me.core + c]

    center = 0.5 * (interval[0] + interval[1])
    half_width = 0.5 * (interval[1] - interval[0])

    def prepare(source, half):
        def tile(i, carry):
            base = half * 1024 + i * 256
            value = source[rows_at(i * 256, 256), :]
            row = me.x * 2048 + base + lax.broadcasted_iota(jnp.int32, (256, 512), 0)
            col = block * 512 + lax.broadcasted_iota(jnp.int32, (256, 512), 1)
            value = jnp.where(row == col, value - center, value) / half_width
            hi, lo = halves(value)
            where = rows_at(base, 256)
            m_hi[where, :] = hi
            m_lo[where, :] = lo
            hi, lo = halves(value.T)
            t_hi[:, where] = hi
            t_lo[:, where] = lo
            return carry

        lax.fori_loop(0, 4, tile, 0)

    prepare(matrix, me.core)
    swap.wait()
    prepare(other, 1 - me.core)
    for d, c, copy in gathers:
        copy.wait()

    def forward(c, f, source, target, before, last=False):
        hi, lo = halves(cols[source, c])
        split_c[c, :, :128] = hi
        split_c[c, :, 128:] = lo
        copies = {}

        def send(q, step, src, dst, link):
            copies[q, step] = remote(src, dst, f_send.at[f, c, q, step], f_recv.at[f, c, q, step], me.partner(link))
            copies[q, step].start()

        where1, where2 = [], []
        for q, (l1, l2, l3, l4) in enumerate(LINKS):
            strip = pl.ds(512 * q, 512)
            both = split_c[c]
            product = dot(m_hi[strip, :], both) + dot(m_lo[strip, :], both)
            part[c, strip, :] = product[:, :128] + product[:, 128:]
            k1, k2 = me.bit(l1), me.bit(l2)
            where1.append(512 * q + 256 * k1)
            where2.append(512 * q + 256 * k1 + 128 * k2)
            send(q, 0, part.at[c, rows_at(512 * q + 256 * (1 - k1), 256)], r1.at[f, c, q], l1)
        yield
        for q, (l1, l2, l3, l4) in enumerate(LINKS):
            k2 = me.bit(l2)
            copies[q, 0].wait_recv()
            h1[c, q] = part[c, rows_at(where1[q], 256), :] + r1[f, c, q]
            send(q, 1, h1.at[c, q, rows_at(128 * (1 - k2), 128)], r2.at[f, c, q], l2)
        yield
        for q, (l1, l2, l3, l4) in enumerate(LINKS):
            k2 = me.bit(l2)
            copies[q, 1].wait_recv()
            h2[c, q] = h1[c, q, rows_at(128 * k2, 128), :] + r2[f, c, q]
            send(q, 2, h2.at[c, q], r3.at[f, c, q], l3)
        yield
        for q, (l1, l2, l3, l4) in enumerate(LINKS):
            copies[q, 2].wait_recv()
            h3[c, q] = h2[c, q] + r3[f, c, q]
            send(q, 3, h3.at[c, q], r4.at[f, c, q], l4)
        yield
        if last:
            for q, (l1, l2, l3, l4) in enumerate(LINKS):
                copies[q, 3].wait_recv()
                share[c, q] = h3[c, q] + r4[f, c, q]
            for copy in copies.values():
                copy.wait_send()
            return
        for q, (l1, l2, l3, l4) in enumerate(LINKS):
            copies[q, 3].wait_recv()
            total = h3[c, q] + r4[f, c, q]
            here = rows_at(where2[q], 128)
            if before is not None:
                total = 2.0 * total - rows[before, c, here, :]
            rows[target, c, here, :] = total
            send(q, 4, rows.at[target, c, here], rows.at[target, c, here], l2)
        yield
        for q, (l1, l2, l3, l4) in enumerate(LINKS):
            copies[q, 4].wait_recv()
            here = rows_at(where1[q], 256)
            send(q, 5, rows.at[target, c, here], rows.at[target, c, here], l1)
        yield
        for q in range(4):
            copies[q, 5].wait_recv()
        for copy in copies.values():
            copy.wait_send()

    def backward(c, b, source, target, before):
        for i in range(4):
            strip = pl.ds(512 * i, 512)
            hi, lo = halves(rows[source, c, strip, :])
            split_r[c, strip, :128] = hi
            split_r[c, strip, 128:] = lo
        orders = ("xa", "xb"), ("xb", "xa")
        copies = {}

        def send(s, step, src, dst, link):
            copies[s, step] = remote(src, dst, b_send.at[b, c, s, step], b_recv.at[b, c, s, step], me.partner(link))
            copies[s, step].start()

        for s in range(2):
            strip = pl.ds(256 * s, 256)
            both = split_r[c]
            product = dot(t_hi[strip, :], both) + dot(t_lo[strip, :], both)
            tb[c, strip, :] = product[:, :128] + product[:, 128:]
            send(s, 0, tb.at[c, strip], rb1.at[b, c, strip], orders[s][0])
        yield
        for s in range(2):
            strip = pl.ds(256 * s, 256)
            copies[s, 0].wait_recv()
            tb2[c, strip, :] = tb[c, strip, :] + rb1[b, c, strip, :]
            send(s, 1, tb2.at[c, strip], rb2.at[b, c, strip], orders[s][1])
        yield
        for s in range(2):
            strip = pl.ds(256 * s, 256)
            copies[s, 1].wait_recv()
            total = tb2[c, strip, :] + rb2[b, c, strip, :]
            if before is not None:
                total = 2.0 * total - cols[before, c, strip, :]
            cols[target, c, strip, :] = total
        for copy in copies.values():
            copy.wait_send()

    def chain(c):
        yield from forward(c, 0, 0, 0, None)
        yield from backward(c, 0, 0, 1, 0)
        yield from forward(c, 1, 1, 1, 0)
        yield from backward(c, 1, 1, 2, None)
        yield from forward(c, 2, 2, 2, 1)
        yield from backward(c, 2, 2, 3, 2)
        yield from forward(c, 3, 3, None, None, last=True)
        pending = []
        for q, (l1, l2, l3, l4) in enumerate(LINKS):
            k1, k2, k3, k4 = me.bit(l1), me.bit(l2), me.bit(l3), me.bit(l4)
            to_x, to_y, to_z = 2 * k1 + k2, q, me.x
            index = 2 * k3 + k4
            same = (to_x == me.x) & (to_y == me.y) & (to_z == me.z)
            there = rows_at(32 * index, 32)
            copy = remote(
                share.at[c, q, there], own3.at[2, c, there],
                p_send.at[c, q], p_recv.at[c, index], me.device(x=to_x, y=to_y, z=to_z),
            )

            @pl.when(jnp.logical_not(same))
            def _():
                copy.start()

            @pl.when(same)
            def _():
                own3[2, c, there, :] = share[c, q, there, :]

            pending.append((same, copy))
        yield
        for same, copy in pending:

            @pl.when(jnp.logical_not(same))
            def _():
                copy.wait_send()

        own_index, own_same = None, None
        for q, (l1, l2, l3, l4) in enumerate(LINKS):
            k1, k2, k3, k4 = me.bit(l1), me.bit(l2), me.bit(l3), me.bit(l4)
            same = (2 * k1 + k2 == me.x) & (q == me.y) & (me.x == me.z)
            own_index = jnp.where(same, 2 * k3 + k4, own_index) if q else jnp.where(same, 2 * k3 + k4, -1)
        for index in range(4):

            @pl.when(own_index != index)
            def _():
                there = pl.ds(32 * index, 32)
                remote(
                    share.at[c, 0, there], own3.at[2, c, there], p_send.at[c, 0], p_recv.at[c, index], me.sibling()
                ).wait_recv()

    left, right = chain(0), chain(1)
    live = [left, right]
    for _ in range(LAG):
        next(left)
    while live:
        for one in list(live):
            if next(one, "end") == "end":
                live.remove(one)

    for c in range(2):
        own3[0, c] = rows[1, c, rows_at(block * 128, 128), :]
        own3[1, c] = cols[3, c, rows_at(me.x * 128, 128), :]
    final = remote(own3, got3, s_send, s_recv, me.sibling())
    final.start()
    final.wait()
    for k, out in enumerate((y3_out, v3_out, z2_out)):
        for c in range(2):

            @pl.when(me.core == 0)
            def _():
                out[:, pl.ds(128 * c, 128)] = own3[k, c]
                out[:, pl.ds(256 + 128 * c, 128)] = got3[k, c]

            @pl.when(me.core == 1)
            def _():
                out[:, pl.ds(128 * c, 128)] = got3[k, c]
                out[:, pl.ds(256 + 128 * c, 128)] = own3[k, c]


LAG = 3


def chain_call(matrix, slab, interval):
    vm = pl.BlockSpec(memory_space=pltpu.VMEM)
    dma = pltpu.SemaphoreType.DMA
    shape = jax.ShapeDtypeStruct((128, 512), F32)
    return pl.pallas_call(
        chain_kernel,
        out_shape=(shape, shape, shape),
        in_specs=[pl.BlockSpec(memory_space=pltpu.SMEM), vm, vm],
        out_specs=(vm, vm, vm),
        scratch_shapes=[
            pltpu.VMEM((1024, 512), F32),
            pltpu.VMEM((2048, 512), BF16),
            pltpu.VMEM((2048, 512), BF16),
            pltpu.VMEM((512, 2048), BF16),
            pltpu.VMEM((512, 2048), BF16),
            pltpu.VMEM((4, 2, 512, 128), F32),
            pltpu.VMEM((3, 2, 2048, 128), F32),
            pltpu.VMEM((2, 2048, 128), F32),
            pltpu.VMEM((2, 512, 256), BF16),
            pltpu.VMEM((2, 2048, 256), BF16),
            pltpu.VMEM((4, 2, 4, 256, 128), F32),
            pltpu.VMEM((2, 4, 256, 128), F32),
            pltpu.VMEM((4, 2, 4, 128, 128), F32),
            pltpu.VMEM((2, 4, 128, 128), F32),
            pltpu.VMEM((4, 2, 4, 128, 128), F32),
            pltpu.VMEM((2, 4, 128, 128), F32),
            pltpu.VMEM((4, 2, 4, 128, 128), F32),
            pltpu.VMEM((2, 4, 128, 128), F32),
            pltpu.VMEM((2, 512, 128), F32),
            pltpu.VMEM((3, 2, 512, 128), F32),
            pltpu.VMEM((2, 512, 128), F32),
            pltpu.VMEM((3, 2, 512, 128), F32),
            pltpu.VMEM((3, 2, 128, 128), F32),
            pltpu.VMEM((3, 2, 128, 128), F32),
            dma((4, 2, 4, 6)),
            dma((4, 2, 4, 6)),
            dma((3, 2, 2, 2)),
            dma((3, 2, 2, 2)),
            dma((8, 2)),
            dma((8, 2)),
            dma,
            dma,
            dma((2, 4)),
            dma((2, 4)),
            dma,
            dma,
        ],
        compiler_params=pltpu.CompilerParams(has_side_effects=True, vmem_limit_bytes=VMEM_LIMIT),
    )(interval, matrix, slab)


def product(left, right):
    return jnp.dot(left, right, precision=lax.Precision.HIGHEST, preferred_element_type=jnp.float32)


def tri_solve(factor, values):
    return jax.scipy.linalg.solve_triangular(factor, values, lower=True)


def shards(matrix, start_vectors, interval):
    pieces = start_vectors.reshape(64, 4, 128).transpose(1, 0, 2)
    total_rows = start_vectors.shape[0] * lax.axis_size(ROW) * lax.axis_size(COL)
    y3, v3, z2 = chain_call(matrix, pieces, interval)
    core = lax.axis_index("row_1")
    mine = lambda a: lax.dynamic_slice_in_dim(a, core * 64, 64, 0)
    y3, v3, z2 = mine(y3), mine(v3), mine(z2)
    first = jnp.linalg.cholesky(lax.psum(product(y3.T, y3), ROW_COL) / total_rows)
    filtered = tri_solve(first, v3.T).T
    mapped = tri_solve(first, z2.T).T
    gram, cross = lax.psum((product(filtered.T, filtered), product(filtered.T, mapped)), ROW_COL)
    factor = jnp.linalg.cholesky(gram / total_rows)
    basis = tri_solve(factor, filtered.T).T
    projected = tri_solve(factor, tri_solve(factor, cross / total_rows).T).T
    residual = tri_solve(factor, mapped.T).T - product(basis, projected)
    return basis, projected, residual


def solution(mesh):
    torus = Mesh(mesh.devices.reshape(4, 2, 4, 4), ("row_0", "row_1", "col_0", "col_1"))
    placed = (P(ROW, COL), P(COL_ROW, None), P())
    return jax.shard_map(
        shards,
        mesh=torus,
        in_specs=placed,
        out_specs=(P(COL_ROW, None), P(), P(COL_ROW, None)),
        check_vma=False,
    )
```

```python
import jax
import jax.numpy as jnp
from jax import lax
from jax.experimental import pallas as pl
from jax.experimental.pallas import tpu as pltpu
from jax.sharding import Mesh
from jax.sharding import PartitionSpec as P

ROW = ("row_0", "row_1")
COL = ("col_0", "col_1")
COL_ROW = ("col_0", "col_1", "row_0", "row_1")
MESH = pl.DeviceIdType.MESH
F32 = jnp.float32
BF16 = jnp.bfloat16
AXES6 = ("xa", "xb", "ya", "yb", "za", "zb"), ("xb", "xa", "yb", "ya", "zb", "za")
SUM_LINKS = tuple(order[k:] + order[:k] for k in (0, 2, 4) for order in AXES6)
SUM_HALF = 48, 48, 40, 40, 40, 40
SUM_START = 0, 96, 192, 272, 352, 432
LAG = 3
VMEM_LIMIT = 63 * 1024 * 1024
LINKS = ("ya", "yb", "za", "zb"), ("yb", "ya", "zb", "za"), ("za", "zb", "ya", "yb"), ("zb", "za", "yb", "ya")


class Place:
    def __init__(self):
        self.x = lax.axis_index("row_0")
        self.core = lax.axis_index("row_1")
        self.z = lax.axis_index("col_0")
        self.y = lax.axis_index("col_1")
        self.at = {"x": self.x, "y": self.y, "z": self.z}

    def device(self, x=None, core=None, z=None, y=None):
        pick = lambda given, own: own if given is None else given
        return (pick(x, self.x), pick(core, self.core), pick(z, self.z), pick(y, self.y))

    def sibling(self):
        return self.device(core=1 - self.core)

    def partner(self, link):
        v = self.at[link[0]]
        w = v + 1 - 2 * (v % 2) if link[1] == "a" else 3 - v
        return self.device(**{link[0]: w})

    def bit(self, link):
        v = self.at[link[0]]
        return ((v + 1) // 2) % 2 if link[1] == "a" else v // 2


def remote(src, dst, send, recv, device):
    return pltpu.make_async_remote_copy(
        src_ref=src, dst_ref=dst, send_sem=send, recv_sem=recv, device_id=device, device_id_type=MESH
    )


def rows_at(start, size):
    return pl.ds(pl.multiple_of(start, size), size)


def lanes_at(start, size):
    return pl.ds(pl.multiple_of(start, 128), size)


def halves(value):
    hi = value.astype(BF16)
    return hi, (value - hi.astype(F32)).astype(BF16)


def dot(left, right):
    return jnp.dot(left, right, preferred_element_type=F32)


def thirds(value):
    a = value.astype(BF16)
    rest = value - a.astype(F32)
    b = rest.astype(BF16)
    return a, b, (rest - b.astype(F32)).astype(BF16)


def small_factor(tile):
    sub = lax.broadcasted_iota(jnp.int32, (8, 128), 0)
    w = [tile[8 * i : 8 * i + 8, :] for i in range(8)]
    for p in range(8):
        col = {(i, c): jnp.broadcast_to(w[i][:, 8 * p + c : 8 * p + c + 1], (8, 128)) for i in range(p, 8) for c in range(8)}
        for c in range(8):
            inv = lax.rsqrt(jnp.broadcast_to(col[p, c][c : c + 1, :], (8, 128)))
            row = jnp.broadcast_to(w[p][c : c + 1, :], (8, 128)) * inv
            own = col[p, c] * inv
            below = sub > c
            w[p] = jnp.where(below, w[p] - own * row, jnp.where(sub == c, row, w[p]))
            steps = [jnp.broadcast_to(own[d : d + 1, :], (8, 128)) for d in range(c + 1, 8)]
            for d in range(c + 1, 8):
                col[p, d] = col[p, d] - own * steps[d - c - 1]
            for i in range(p + 1, 8):
                mult = col[i, c] * inv
                w[i] = w[i] - mult * row
                for d in range(c + 1, 8):
                    col[i, d] = col[i, d] - mult * steps[d - c - 1]
    return jnp.concatenate(w, axis=0)


def factor_blocks(x, first, last):
    def block(k, carry):
        here = pl.ds(pl.multiple_of(64 * k, 64), 64)
        pair = pl.ds(pl.multiple_of(128 * (k // 2), 128), 128)
        odd = k % 2
        lane = lax.broadcasted_iota(jnp.int32, (64, 128), 1)
        rowi = lax.broadcasted_iota(jnp.int32, (64, 128), 0)
        a = x[here, pair]
        a = jnp.where(odd == 1, pltpu.roll(a, 64, 1), a)
        w = small_factor(jnp.where(lane < 64, a, (lane - 64 == rowi).astype(F32)))
        linv = pltpu.roll(w, 64, 1)[:, :64]
        rows = jnp.dot(linv, x[here, :], precision=lax.Precision.HIGHEST, preferred_element_type=F32)
        x[here, :] = rows
        placed = jnp.where(odd == 1, w, pltpu.roll(w, 64, 1))
        x[here, pair] = jnp.where(lane // 64 == odd, placed, x[here, pair])
        full = x[here, :]
        wide = lax.broadcasted_iota(jnp.int32, (64, 512), 1)
        left = jnp.where(wide // 64 > k, full, 0.0)
        h, m, l = thirds(full)
        lh, lm, ll = thirds(left)
        right = jnp.concatenate([h, m, h, m, l, h], axis=0)
        lefts = jnp.concatenate([lh, lh, lm, lm, lh, ll], axis=0)
        for i in range(4):
            strip = pl.ds(128 * i, 128)
            update = lax.dot_general(
                lefts[:, 128 * i : 128 * i + 128], right, (((0,), (0,)), ((), ())), preferred_element_type=F32
            )
            r = 128 * i + lax.broadcasted_iota(jnp.int32, (128, 512), 0)
            c = lax.broadcasted_iota(jnp.int32, (128, 512), 1)
            x[strip, :] = jnp.where((c // 64 == k) & (r // 64 > k), 0.0, x[strip, :]) - update
        return carry

    lax.fori_loop(first, last, block, 0)


def lower_only(x):
    for i in range(4):
        strip = pl.ds(128 * i, 128)
        r = 128 * i + lax.broadcasted_iota(jnp.int32, (128, 512), 0)
        c = lax.broadcasted_iota(jnp.int32, (128, 512), 1)
        x[strip, :] = jnp.where(c <= r, x[strip, :], 0.0)


def exact(left, right, dims=((1,), (0,))):
    return lax.dot_general(
        left, right, (dims, ((), ())), precision=lax.Precision.HIGHEST, preferred_element_type=F32
    )


def chain_kernel(
    interval, matrix, slab, basis_out, proj_out, resid_out,
    other, m_hi, m_lo, t_hi, t_lo, cols, rows, part, split_c, split_r,
    r1, h1, r2, h2, r3, h3, r4, share,
    tb, rb1, tb2, rb2, full, mapped, local, total, term, got, inverse, cross,
    f_send, f_recv, b_send, b_recv, g_send, g_recv, m_send, m_recv, p_send, p_recv, s_send, s_recv,
    a_send, a_recv, x_send, x_recv,
):
    me = Place()
    block = me.z * 4 + me.y

    swap = remote(matrix, other, m_send, m_recv, me.sibling())
    swap.start()

    def slab_rows(x, core):
        return rows_at((x * 2 + core) * 64, 64)

    gathers = []
    for d in range(1, 8):
        to_x, to_core = (me.x + d // 2) % 4, (me.core + d) % 2
        for c in range(2):
            copy = remote(
                slab.at[:, lanes_at(256 * to_core + 128 * c, 128)], cols.at[0, c, slab_rows(me.x, me.core)],
                g_send.at[d, c], g_recv.at[d, c], me.device(x=to_x, core=to_core),
            )
            copy.start()
            gathers.append((d, c, copy))
    for c in range(2):
        cols[0, c, slab_rows(me.x, me.core), :] = slab[:, lanes_at(256 * me.core + 128 * c, 128)]

    center = 0.5 * (interval[0] + interval[1])
    half_width = 0.5 * (interval[1] - interval[0])

    def prepare(source, half):
        def tile(i, carry):
            base = half * 1024 + i * 256
            value = source[rows_at(i * 256, 256), :]
            row = me.x * 2048 + base + lax.broadcasted_iota(jnp.int32, (256, 512), 0)
            col = block * 512 + lax.broadcasted_iota(jnp.int32, (256, 512), 1)
            value = jnp.where(row == col, value - center, value) / half_width
            hi, lo = halves(value)
            where = rows_at(base, 256)
            m_hi[where, :] = hi
            m_lo[where, :] = lo
            hi, lo = halves(value.T)
            t_hi[:, where] = hi
            t_lo[:, where] = lo
            return carry

        lax.fori_loop(0, 4, tile, 0)

    prepare(matrix, me.core)
    swap.wait()
    prepare(other, 1 - me.core)
    for d, c, copy in gathers:
        copy.wait()

    def forward(c, f, source, target, before, last=False):
        hi, lo = halves(cols[source, c])
        split_c[c, :, :128] = hi
        split_c[c, :, 128:] = lo
        copies = {}

        def send(q, step, src, dst, link):
            copies[q, step] = remote(src, dst, f_send.at[f, c, q, step], f_recv.at[f, c, q, step], me.partner(link))
            copies[q, step].start()

        where1, where2 = [], []
        for q, (l1, l2, l3, l4) in enumerate(LINKS):
            strip = pl.ds(512 * q, 512)
            both = split_c[c]
            product = dot(m_hi[strip, :], both) + dot(m_lo[strip, :], both)
            part[c, strip, :] = product[:, :128] + product[:, 128:]
            k1, k2 = me.bit(l1), me.bit(l2)
            where1.append(512 * q + 256 * k1)
            where2.append(512 * q + 256 * k1 + 128 * k2)
            send(q, 0, part.at[c, rows_at(512 * q + 256 * (1 - k1), 256)], r1.at[f, c, q], l1)
        yield
        for q, (l1, l2, l3, l4) in enumerate(LINKS):
            k2 = me.bit(l2)
            copies[q, 0].wait_recv()
            h1[c, q] = part[c, rows_at(where1[q], 256), :] + r1[f, c, q]
            send(q, 1, h1.at[c, q, rows_at(128 * (1 - k2), 128)], r2.at[f, c, q], l2)
        yield
        for q, (l1, l2, l3, l4) in enumerate(LINKS):
            k2 = me.bit(l2)
            copies[q, 1].wait_recv()
            h2[c, q] = h1[c, q, rows_at(128 * k2, 128), :] + r2[f, c, q]
            send(q, 2, h2.at[c, q], r3.at[f, c, q], l3)
        yield
        for q, (l1, l2, l3, l4) in enumerate(LINKS):
            copies[q, 2].wait_recv()
            h3[c, q] = h2[c, q] + r3[f, c, q]
            send(q, 3, h3.at[c, q], r4.at[f, c, q], l4)
        yield
        if last:
            for q, (l1, l2, l3, l4) in enumerate(LINKS):
                copies[q, 3].wait_recv()
                share[c, q] = h3[c, q] + r4[f, c, q]
            for copy in copies.values():
                copy.wait_send()
            return
        for q, (l1, l2, l3, l4) in enumerate(LINKS):
            copies[q, 3].wait_recv()
            total = h3[c, q] + r4[f, c, q]
            here = rows_at(where2[q], 128)
            if before is not None:
                total = 2.0 * total - rows[before, c, here, :]
            rows[target, c, here, :] = total
            send(q, 4, rows.at[target, c, here], rows.at[target, c, here], l2)
        yield
        for q, (l1, l2, l3, l4) in enumerate(LINKS):
            copies[q, 4].wait_recv()
            here = rows_at(where1[q], 256)
            send(q, 5, rows.at[target, c, here], rows.at[target, c, here], l1)
        yield
        for q in range(4):
            copies[q, 5].wait_recv()
        for copy in copies.values():
            copy.wait_send()

    def backward(c, b, source, target, before):
        for i in range(4):
            strip = pl.ds(512 * i, 512)
            hi, lo = halves(rows[source, c, strip, :])
            split_r[c, strip, :128] = hi
            split_r[c, strip, 128:] = lo
        orders = ("xa", "xb"), ("xb", "xa")
        copies = {}

        def send(s, step, src, dst, link):
            copies[s, step] = remote(src, dst, b_send.at[b, c, s, step], b_recv.at[b, c, s, step], me.partner(link))
            copies[s, step].start()

        for s in range(2):
            strip = pl.ds(256 * s, 256)
            both = split_r[c]
            product = dot(t_hi[strip, :], both) + dot(t_lo[strip, :], both)
            tb[c, strip, :] = product[:, :128] + product[:, 128:]
            send(s, 0, tb.at[c, strip], rb1.at[b, c, strip], orders[s][0])
        yield
        for s in range(2):
            strip = pl.ds(256 * s, 256)
            copies[s, 0].wait_recv()
            tb2[c, strip, :] = tb[c, strip, :] + rb1[b, c, strip, :]
            send(s, 1, tb2.at[c, strip], rb2.at[b, c, strip], orders[s][1])
        yield
        for s in range(2):
            strip = pl.ds(256 * s, 256)
            copies[s, 1].wait_recv()
            total = tb2[c, strip, :] + rb2[b, c, strip, :]
            if before is not None:
                total = 2.0 * total - cols[before, c, strip, :]
            cols[target, c, strip, :] = total
        for copy in copies.values():
            copy.wait_send()

    done = set()

    def chain(c):
        yield from forward(c, 0, 0, 0, None)
        yield from backward(c, 0, 0, 1, 0)
        yield from forward(c, 1, 1, 1, 0)
        done.add(("y3", c))
        yield from backward(c, 1, 1, 2, None)
        yield from forward(c, 2, 2, 2, 1)
        yield from backward(c, 2, 2, 3, 2)
        done.add(("v3", c))
        yield from forward(c, 3, 3, None, None, last=True)
        mine = lanes_at(256 * me.core + 128 * c, 128)
        pending = []
        own_index = None
        for q, (l1, l2, l3, l4) in enumerate(LINKS):
            k1, k2, k3, k4 = me.bit(l1), me.bit(l2), me.bit(l3), me.bit(l4)
            to_x, to_y, to_z = 2 * k1 + k2, q, me.x
            index = 2 * k3 + k4
            same = (to_x == me.x) & (to_y == me.y) & (to_z == me.z)
            own_index = jnp.where(same, index, -1 if own_index is None else own_index)
            there = rows_at(32 * index, 32)
            copy = remote(
                share.at[c, q, there], full.at[2, there, mine],
                p_send.at[c, q], p_recv.at[c, index], me.device(x=to_x, y=to_y, z=to_z),
            )

            @pl.when(jnp.logical_not(same))
            def _():
                copy.start()

            @pl.when(same)
            def _():
                full[2, there, mine] = share[c, q, there, :]

            pending.append((same, copy))
        yield
        for same, copy in pending:

            @pl.when(jnp.logical_not(same))
            def _():
                copy.wait_send()

        for index in range(4):

            @pl.when(own_index != index)
            def _():
                there = pl.ds(32 * index, 32)
                remote(
                    share.at[c, 0, there], full.at[2, there, mine], p_send.at[c, 0], p_recv.at[c, index], me.sibling()
                ).wait_recv()

        done.add(("z2", c))

    half = lanes_at(256 * me.core, 256)

    def needs(*marks):
        while not all(mark in done for mark in marks):
            yield "blocked"

    def swap_slab(k):
        copy = remote(full.at[k, :, half], full.at[k, :, half], s_send.at[k], s_recv.at[k], me.sibling())
        copy.start()
        yield
        copy.wait()

    def all_sum(n, target):
        copies = {}

        def send(s, t, src, dst, link):
            copies[s, t] = remote(src, dst, a_send.at[n, s, t], a_recv.at[n, s, t], me.partner(link))
            copies[s, t].start()

        def piece(s, k):
            return pl.ds(pl.multiple_of(SUM_START[s] + SUM_HALF[s] * k, 8), SUM_HALF[s])

        for s, order in enumerate(SUM_LINKS):
            small = pl.ds(0, SUM_HALF[s])
            send(s, 0, local.at[n, piece(s, 1 - me.bit(order[0]))], got.at[n, 0, s, small], order[0])
        yield
        for t in range(1, 6):
            for s, order in enumerate(SUM_LINKS):
                small = pl.ds(0, SUM_HALF[s])
                copies[s, t - 1].wait_recv()
                before = local[n, piece(s, me.bit(order[0])), :] if t == 1 else term[n % 2, t - 2, s, small, :]
                term[n % 2, t - 1, s, small, :] = before + got[n, t - 1, s, small, :]
                send(s, t, term.at[n % 2, t - 1, s, small], got.at[n, t, s, small], order[t])
            yield
        for s, order in enumerate(SUM_LINKS):
            small = pl.ds(0, SUM_HALF[s])
            copies[s, 5].wait_recv()
            here = piece(s, me.bit(order[0]))
            total[n, here, :] = term[n % 2, 4, s, small, :] + got[n, 5, s, small, :]
            send(s, 6, total.at[n, here], total.at[n, here], order[0])
        yield
        for s in range(6):
            copies[s, 6].wait_recv()
        copy = remote(total.at[n], target.at[:, half], x_send.at[n], x_recv.at[n], me.sibling())
        copy.start()
        target[:, half] = total[n]
        for one in copies.values():
            one.wait_send()
        yield
        copy.wait()

    def first_factor():
        yield from needs(("y3", 0), ("y3", 1))
        for c in range(2):
            full[0, :, lanes_at(256 * me.core + 128 * c, 128)] = rows[1, c, rows_at(block * 128, 128), :]
        yield from swap_slab(0)
        local[0] = exact(full[0], full[0, :, half], ((0,), (0,))) / 8192
        yield from all_sum(0, inverse.at[0])
        for k in range(0, 8, 2):
            factor_blocks(inverse.at[0], k, k + 2)
            yield
        lower_only(inverse.at[0])
        done.add("first")

    def second_factor():
        yield from needs(("v3", 0), ("v3", 1))
        for c in range(2):
            full[1, :, lanes_at(256 * me.core + 128 * c, 128)] = cols[3, c, rows_at(me.x * 128, 128), :]
        yield from swap_slab(1)
        yield from needs("first")
        mapped[0] = exact(full[1], inverse[0], ((1,), (1,)))
        local[1] = exact(mapped[0], mapped[0, :, half], ((0,), (0,))) / 8192
        done.add("filtered")
        yield from all_sum(1, inverse.at[1])
        for k in range(0, 8, 2):
            factor_blocks(inverse.at[1], k, k + 2)
            yield
        lower_only(inverse.at[1])
        done.add("second")

    def cross_terms():
        yield from needs(("z2", 0), ("z2", 1), "filtered")
        yield from swap_slab(2)
        mapped[1] = exact(full[2], inverse[0], ((1,), (1,)))
        local[2] = exact(mapped[0], mapped[1, :, half], ((0,), (0,))) / 8192
        yield from all_sum(2, cross)

    live = [chain(0), chain(1), first_factor(), second_factor(), cross_terms()]
    for _ in range(LAG):
        next(live[0])
    while live:
        for one in list(live):
            if next(one, "end") == "end":
                live.remove(one)

    mine = rows_at(64 * me.core, 64)
    basis = exact(mapped[0, mine, :], inverse[1], ((1,), (1,)))
    basis_out[...] = basis
    cross[...] = exact(inverse[1], cross[...])
    proj_out[...] = exact(cross[...], inverse[1], ((1,), (1,)))
    resid_out[...] = exact(mapped[1, mine, :], inverse[1], ((1,), (1,))) - exact(basis, proj_out[...])


def chain_call(matrix, slab, interval):
    vm = pl.BlockSpec(memory_space=pltpu.VMEM)
    dma = pltpu.SemaphoreType.DMA
    slab_shape = jax.ShapeDtypeStruct((64, 512), F32)
    return pl.pallas_call(
        chain_kernel,
        out_shape=(slab_shape, jax.ShapeDtypeStruct((512, 512), F32), slab_shape),
        in_specs=[pl.BlockSpec(memory_space=pltpu.SMEM), vm, vm],
        out_specs=(vm, vm, vm),
        scratch_shapes=[
            pltpu.VMEM((1024, 512), F32),
            pltpu.VMEM((2048, 512), BF16),
            pltpu.VMEM((2048, 512), BF16),
            pltpu.VMEM((512, 2048), BF16),
            pltpu.VMEM((512, 2048), BF16),
            pltpu.VMEM((4, 2, 512, 128), F32),
            pltpu.VMEM((3, 2, 2048, 128), F32),
            pltpu.VMEM((2, 2048, 128), F32),
            pltpu.VMEM((2, 512, 256), BF16),
            pltpu.VMEM((2, 2048, 256), BF16),
            pltpu.VMEM((4, 2, 4, 256, 128), F32),
            pltpu.VMEM((2, 4, 256, 128), F32),
            pltpu.VMEM((4, 2, 4, 128, 128), F32),
            pltpu.VMEM((2, 4, 128, 128), F32),
            pltpu.VMEM((4, 2, 4, 128, 128), F32),
            pltpu.VMEM((2, 4, 128, 128), F32),
            pltpu.VMEM((4, 2, 4, 128, 128), F32),
            pltpu.VMEM((2, 4, 128, 128), F32),
            pltpu.VMEM((2, 512, 128), F32),
            pltpu.VMEM((3, 2, 512, 128), F32),
            pltpu.VMEM((2, 512, 128), F32),
            pltpu.VMEM((3, 2, 512, 128), F32),
            pltpu.VMEM((3, 128, 512), F32),
            pltpu.VMEM((2, 128, 512), F32),
            pltpu.VMEM((3, 512, 256), F32),
            pltpu.VMEM((3, 512, 256), F32),
            pltpu.VMEM((2, 5, 6, 48, 256), F32),
            pltpu.VMEM((3, 6, 6, 48, 256), F32),
            pltpu.VMEM((2, 512, 512), F32),
            pltpu.VMEM((512, 512), F32),
            dma((4, 2, 4, 6)),
            dma((4, 2, 4, 6)),
            dma((3, 2, 2, 2)),
            dma((3, 2, 2, 2)),
            dma((8, 2)),
            dma((8, 2)),
            dma,
            dma,
            dma((2, 4)),
            dma((2, 4)),
            dma((3,)),
            dma((3,)),
            dma((3, 6, 7)),
            dma((3, 6, 7)),
            dma((3,)),
            dma((3,)),
        ],
        compiler_params=pltpu.CompilerParams(has_side_effects=True, vmem_limit_bytes=VMEM_LIMIT),
    )(interval, matrix, slab)


def shards(matrix, start_vectors, interval):
    return chain_call(matrix, start_vectors, interval)


def solution(mesh):
    torus = Mesh(mesh.devices.reshape(4, 2, 4, 4), ("row_0", "row_1", "col_0", "col_1"))
    placed = (P(ROW, COL), P(COL_ROW, None), P())
    return jax.shard_map(
        shards,
        mesh=torus,
        in_specs=placed,
        out_specs=(P(COL_ROW, None), P(), P(COL_ROW, None)),
        check_vma=False,
    )
```

```python
import jax
import jax.numpy as jnp
from jax import lax
from jax.experimental import pallas as pl
from jax.experimental.pallas import tpu as pltpu
from jax.sharding import Mesh
from jax.sharding import PartitionSpec as P

ROW = ("row_0", "row_1")
COL = ("col_0", "col_1")
COL_ROW = ("col_0", "col_1", "row_0", "row_1")
MESH = pl.DeviceIdType.MESH
F32 = jnp.float32
BF16 = jnp.bfloat16
AXES6 = ("xa", "xb", "ya", "yb", "za", "zb"), ("xb", "xa", "yb", "ya", "zb", "za")
SUM_LINKS = tuple(order[k:] + order[:k] for k in (0, 2, 4) for order in AXES6)
SUM_HALF = 48, 48, 40, 40, 40, 40
SUM_START = 0, 96, 192, 272, 352, 432
VMEM_LIMIT = 63 * 1024 * 1024
LINKS = ("ya", "yb", "za", "zb"), ("yb", "ya", "zb", "za"), ("za", "zb", "ya", "yb"), ("zb", "za", "yb", "ya")


class Place:
    def __init__(self):
        self.x = lax.axis_index("row_0")
        self.core = lax.axis_index("row_1")
        self.z = lax.axis_index("col_0")
        self.y = lax.axis_index("col_1")
        self.at = {"x": self.x, "y": self.y, "z": self.z}

    def device(self, x=None, core=None, z=None, y=None):
        pick = lambda given, own: own if given is None else given
        return (pick(x, self.x), pick(core, self.core), pick(z, self.z), pick(y, self.y))

    def sibling(self):
        return self.device(core=1 - self.core)

    def partner(self, link):
        v = self.at[link[0]]
        w = v + 1 - 2 * (v % 2) if link[1] == "a" else 3 - v
        return self.device(**{link[0]: w})

    def bit(self, link):
        v = self.at[link[0]]
        return ((v + 1) // 2) % 2 if link[1] == "a" else v // 2


def remote(src, dst, send, recv, device):
    return pltpu.make_async_remote_copy(
        src_ref=src, dst_ref=dst, send_sem=send, recv_sem=recv, device_id=device, device_id_type=MESH
    )


def rows_at(start, size):
    return pl.ds(pl.multiple_of(start, size), size)


def lanes_at(start, size):
    return pl.ds(pl.multiple_of(start, 128), size)


def halves(value):
    hi = value.astype(BF16)
    return hi, (value - hi.astype(F32)).astype(BF16)


def dot(left, right):
    return jnp.dot(left, right, preferred_element_type=F32)


def thirds(value):
    a = value.astype(BF16)
    rest = value - a.astype(F32)
    b = rest.astype(BF16)
    return a, b, (rest - b.astype(F32)).astype(BF16)


def small_factor(tile):
    sub = lax.broadcasted_iota(jnp.int32, (8, 128), 0)
    w = [tile[8 * i : 8 * i + 8, :] for i in range(8)]
    for p in range(8):
        col = {(i, c): jnp.broadcast_to(w[i][:, 8 * p + c : 8 * p + c + 1], (8, 128)) for i in range(p, 8) for c in range(8)}
        for c in range(8):
            inv = lax.rsqrt(jnp.broadcast_to(col[p, c][c : c + 1, :], (8, 128)))
            row = jnp.broadcast_to(w[p][c : c + 1, :], (8, 128)) * inv
            own = col[p, c] * inv
            below = sub > c
            w[p] = jnp.where(below, w[p] - own * row, jnp.where(sub == c, row, w[p]))
            steps = [jnp.broadcast_to(own[d : d + 1, :], (8, 128)) for d in range(c + 1, 8)]
            for d in range(c + 1, 8):
                col[p, d] = col[p, d] - own * steps[d - c - 1]
            for i in range(p + 1, 8):
                mult = col[i, c] * inv
                w[i] = w[i] - mult * row
                for d in range(c + 1, 8):
                    col[i, d] = col[i, d] - mult * steps[d - c - 1]
    return jnp.concatenate(w, axis=0)


def factor_blocks(x, first, last):
    def block(k, carry):
        here = pl.ds(pl.multiple_of(64 * k, 64), 64)
        pair = pl.ds(pl.multiple_of(128 * (k // 2), 128), 128)
        odd = k % 2
        lane = lax.broadcasted_iota(jnp.int32, (64, 128), 1)
        rowi = lax.broadcasted_iota(jnp.int32, (64, 128), 0)
        a = x[here, pair]
        a = jnp.where(odd == 1, pltpu.roll(a, 64, 1), a)
        w = small_factor(jnp.where(lane < 64, a, (lane - 64 == rowi).astype(F32)))
        linv = pltpu.roll(w, 64, 1)[:, :64]
        rows = jnp.dot(linv, x[here, :], precision=lax.Precision.HIGHEST, preferred_element_type=F32)
        x[here, :] = rows
        placed = jnp.where(odd == 1, w, pltpu.roll(w, 64, 1))
        x[here, pair] = jnp.where(lane // 64 == odd, placed, x[here, pair])
        full = x[here, :]
        wide = lax.broadcasted_iota(jnp.int32, (64, 512), 1)
        left = jnp.where(wide // 64 > k, full, 0.0)
        h, m, l = thirds(full)
        lh, lm, ll = thirds(left)
        right = jnp.concatenate([h, m, h, m, l, h], axis=0)
        lefts = jnp.concatenate([lh, lh, lm, lm, lh, ll], axis=0)
        for i in range(4):
            strip = pl.ds(128 * i, 128)
            update = lax.dot_general(
                lefts[:, 128 * i : 128 * i + 128], right, (((0,), (0,)), ((), ())), preferred_element_type=F32
            )
            r = 128 * i + lax.broadcasted_iota(jnp.int32, (128, 512), 0)
            c = lax.broadcasted_iota(jnp.int32, (128, 512), 1)
            x[strip, :] = jnp.where((c // 64 == k) & (r // 64 > k), 0.0, x[strip, :]) - update
        return carry

    lax.fori_loop(first, last, block, 0)


def lower_only(x):
    for i in range(4):
        strip = pl.ds(128 * i, 128)
        r = 128 * i + lax.broadcasted_iota(jnp.int32, (128, 512), 0)
        c = lax.broadcasted_iota(jnp.int32, (128, 512), 1)
        x[strip, :] = jnp.where(c <= r, x[strip, :], 0.0)


def exact(left, right, dims=((1,), (0,))):
    return lax.dot_general(
        left, right, (dims, ((), ())), precision=lax.Precision.HIGHEST, preferred_element_type=F32
    )


def chain_kernel(
    interval, matrix, slab, basis_out, proj_out, resid_out,
    other, m_hi, m_lo, t_hi, t_lo, cols, rows, part, split_c, split_r,
    r1, h1, r2, h2, r3, h3, r4, share,
    tb, rb1, tb2, rb2, full, mapped, local, total, term, got, inverse, cross,
    f_send, f_recv, b_send, b_recv, g_send, g_recv, m_send, m_recv, p_send, p_recv, s_send, s_recv,
    a_send, a_recv, x_send, x_recv,
):
    me = Place()
    block = me.z * 4 + me.y

    barrier = pltpu.get_barrier_semaphore()
    near = [me.device(x=(me.x + d // 2) % 4, core=(me.core + d) % 2) for d in range(1, 8)]
    near += [me.partner(link) for link in ("ya", "yb", "za", "zb")]
    for device in near:
        pl.semaphore_signal(barrier, inc=1, device_id=device, device_id_type=MESH)
    pl.semaphore_wait(barrier, len(near))

    swap = remote(matrix, other, m_send, m_recv, me.sibling())
    swap.start()

    def slab_rows(x, core):
        return rows_at((x * 2 + core) * 64, 64)

    gathers = []
    for d in range(1, 8):
        to_x, to_core = (me.x + d // 2) % 4, (me.core + d) % 2
        for c in range(2):
            copy = remote(
                slab.at[:, lanes_at(256 * to_core + 128 * c, 128)], cols.at[0, c, slab_rows(me.x, me.core)],
                g_send.at[d, c], g_recv.at[d, c], me.device(x=to_x, core=to_core),
            )
            copy.start()
            gathers.append((d, c, copy))
    for c in range(2):
        cols[0, c, slab_rows(me.x, me.core), :] = slab[:, lanes_at(256 * me.core + 128 * c, 128)]

    center = 0.5 * (interval[0] + interval[1])
    half_width = 0.5 * (interval[1] - interval[0])

    def prepare(source, half):
        def tile(i, carry):
            base = half * 1024 + i * 256
            value = source[rows_at(i * 256, 256), :]
            row = me.x * 2048 + base + lax.broadcasted_iota(jnp.int32, (256, 512), 0)
            col = block * 512 + lax.broadcasted_iota(jnp.int32, (256, 512), 1)
            value = jnp.where(row == col, value - center, value) / half_width
            hi, lo = halves(value)
            where = rows_at(base, 256)
            m_hi[where, :] = hi
            m_lo[where, :] = lo
            hi, lo = halves(value.T)
            t_hi[:, where] = hi
            t_lo[:, where] = lo
            return carry

        lax.fori_loop(0, 4, tile, 0)

    prepare(matrix, me.core)
    swap.wait()
    prepare(other, 1 - me.core)
    for d, c, copy in gathers:
        copy.wait()

    def forward(c, f, source, target, before, last=False):
        hi, lo = halves(cols[source, c])
        split_c[c, :, :128] = hi
        split_c[c, :, 128:] = lo
        copies = {}

        def send(q, step, src, dst, link):
            copies[q, step] = remote(src, dst, f_send.at[f, c, q, step], f_recv.at[f, c, q, step], me.partner(link))
            copies[q, step].start()

        where1, where2 = [], []
        for q, (l1, l2, l3, l4) in enumerate(LINKS):
            strip = pl.ds(512 * q, 512)
            both = split_c[c]
            product = dot(m_hi[strip, :], both) + dot(m_lo[strip, :], both)
            part[c, strip, :] = product[:, :128] + product[:, 128:]
            k1, k2 = me.bit(l1), me.bit(l2)
            where1.append(512 * q + 256 * k1)
            where2.append(512 * q + 256 * k1 + 128 * k2)
            send(q, 0, part.at[c, rows_at(512 * q + 256 * (1 - k1), 256)], r1.at[f, c, q], l1)
        yield
        for q, (l1, l2, l3, l4) in enumerate(LINKS):
            k2 = me.bit(l2)
            copies[q, 0].wait_recv()
            h1[c, q] = part[c, rows_at(where1[q], 256), :] + r1[f, c, q]
            send(q, 1, h1.at[c, q, rows_at(128 * (1 - k2), 128)], r2.at[f, c, q], l2)
        yield
        for q, (l1, l2, l3, l4) in enumerate(LINKS):
            k2 = me.bit(l2)
            copies[q, 1].wait_recv()
            h2[c, q] = h1[c, q, rows_at(128 * k2, 128), :] + r2[f, c, q]
            send(q, 2, h2.at[c, q], r3.at[f, c, q], l3)
        yield
        for q, (l1, l2, l3, l4) in enumerate(LINKS):
            copies[q, 2].wait_recv()
            h3[c, q] = h2[c, q] + r3[f, c, q]
            send(q, 3, h3.at[c, q], r4.at[f, c, q], l4)
        yield
        if last:
            for q, (l1, l2, l3, l4) in enumerate(LINKS):
                copies[q, 3].wait_recv()
                share[c, q] = h3[c, q] + r4[f, c, q]
            for copy in copies.values():
                copy.wait_send()
            return
        for q, (l1, l2, l3, l4) in enumerate(LINKS):
            copies[q, 3].wait_recv()
            total = h3[c, q] + r4[f, c, q]
            here = rows_at(where2[q], 128)
            if before is not None:
                total = 2.0 * total - rows[before, c, here, :]
            rows[target, c, here, :] = total
            send(q, 4, rows.at[target, c, here], rows.at[target, c, here], l2)
        yield
        for q, (l1, l2, l3, l4) in enumerate(LINKS):
            copies[q, 4].wait_recv()
            here = rows_at(where1[q], 256)
            send(q, 5, rows.at[target, c, here], rows.at[target, c, here], l1)
        yield
        for q in range(4):
            copies[q, 5].wait_recv()
        for copy in copies.values():
            copy.wait_send()

    def backward(c, b, source, target, before):
        for i in range(4):
            strip = pl.ds(512 * i, 512)
            hi, lo = halves(rows[source, c, strip, :])
            split_r[c, strip, :128] = hi
            split_r[c, strip, 128:] = lo
        orders = ("xa", "xb"), ("xb", "xa")
        copies = {}

        def send(s, step, src, dst, link):
            copies[s, step] = remote(src, dst, b_send.at[b, c, s, step], b_recv.at[b, c, s, step], me.partner(link))
            copies[s, step].start()

        for s in range(2):
            strip = pl.ds(256 * s, 256)
            both = split_r[c]
            product = dot(t_hi[strip, :], both) + dot(t_lo[strip, :], both)
            tb[c, strip, :] = product[:, :128] + product[:, 128:]
            send(s, 0, tb.at[c, strip], rb1.at[b, c, strip], orders[s][0])
        yield
        for s in range(2):
            strip = pl.ds(256 * s, 256)
            copies[s, 0].wait_recv()
            tb2[c, strip, :] = tb[c, strip, :] + rb1[b, c, strip, :]
            send(s, 1, tb2.at[c, strip], rb2.at[b, c, strip], orders[s][1])
        yield
        for s in range(2):
            strip = pl.ds(256 * s, 256)
            copies[s, 1].wait_recv()
            total = tb2[c, strip, :] + rb2[b, c, strip, :]
            if before is not None:
                total = 2.0 * total - cols[before, c, strip, :]
            cols[target, c, strip, :] = total
        for copy in copies.values():
            copy.wait_send()

    done = set()

    def chain(c):
        yield from forward(c, 0, 0, 0, None)
        yield from backward(c, 0, 0, 1, 0)
        yield from forward(c, 1, 1, 1, 0)
        done.add(("y3", c))
        yield from backward(c, 1, 1, 2, None)
        yield from forward(c, 2, 2, 2, 1)
        yield from backward(c, 2, 2, 3, 2)
        done.add(("v3", c))
        yield from forward(c, 3, 3, None, None, last=True)
        mine = lanes_at(256 * me.core + 128 * c, 128)
        pending = []
        own_index = None
        for q, (l1, l2, l3, l4) in enumerate(LINKS):
            k1, k2, k3, k4 = me.bit(l1), me.bit(l2), me.bit(l3), me.bit(l4)
            to_x, to_y, to_z = 2 * k1 + k2, q, me.x
            index = 2 * k3 + k4
            same = (to_x == me.x) & (to_y == me.y) & (to_z == me.z)
            own_index = jnp.where(same, index, -1 if own_index is None else own_index)
            there = rows_at(32 * index, 32)
            copy = remote(
                share.at[c, q, there], full.at[2, there, mine],
                p_send.at[c, q], p_recv.at[c, index], me.device(x=to_x, y=to_y, z=to_z),
            )

            @pl.when(jnp.logical_not(same))
            def _():
                copy.start()

            @pl.when(same)
            def _():
                full[2, there, mine] = share[c, q, there, :]

            pending.append((same, copy))
        yield
        for same, copy in pending:

            @pl.when(jnp.logical_not(same))
            def _():
                copy.wait_send()

        for index in range(4):

            @pl.when(own_index != index)
            def _():
                there = pl.ds(32 * index, 32)
                remote(
                    share.at[c, 0, there], full.at[2, there, mine], p_send.at[c, 0], p_recv.at[c, index], me.sibling()
                ).wait_recv()

        done.add(("z2", c))

    half = lanes_at(256 * me.core, 256)

    def needs(*marks):
        while not all(mark in done for mark in marks):
            yield "blocked"

    def swap_slab(k):
        copy = remote(full.at[k, :, half], full.at[k, :, half], s_send.at[k], s_recv.at[k], me.sibling())
        copy.start()
        yield
        copy.wait()

    def all_sum(n, target):
        copies = {}

        def send(s, t, src, dst, link):
            copies[s, t] = remote(src, dst, a_send.at[n, s, t], a_recv.at[n, s, t], me.partner(link))
            copies[s, t].start()

        def piece(s, k):
            return pl.ds(pl.multiple_of(SUM_START[s] + SUM_HALF[s] * k, 8), SUM_HALF[s])

        for s, order in enumerate(SUM_LINKS):
            small = pl.ds(0, SUM_HALF[s])
            send(s, 0, local.at[n, piece(s, 1 - me.bit(order[0]))], got.at[n, 0, s, small], order[0])
        yield
        for t in range(1, 6):
            for s, order in enumerate(SUM_LINKS):
                small = pl.ds(0, SUM_HALF[s])
                copies[s, t - 1].wait_recv()
                before = local[n, piece(s, me.bit(order[0])), :] if t == 1 else term[n % 2, t - 2, s, small, :]
                term[n % 2, t - 1, s, small, :] = before + got[n, t - 1, s, small, :]
                send(s, t, term.at[n % 2, t - 1, s, small], got.at[n, t, s, small], order[t])
            yield
        for s, order in enumerate(SUM_LINKS):
            small = pl.ds(0, SUM_HALF[s])
            copies[s, 5].wait_recv()
            here = piece(s, me.bit(order[0]))
            total[n, here, :] = term[n % 2, 4, s, small, :] + got[n, 5, s, small, :]
            send(s, 6, total.at[n, here], total.at[n, here], order[0])
        yield
        for s in range(6):
            copies[s, 6].wait_recv()
        copy = remote(total.at[n], target.at[:, half], x_send.at[n], x_recv.at[n], me.sibling())
        copy.start()
        target[:, half] = total[n]
        for one in copies.values():
            one.wait_send()
        yield
        copy.wait()

    def first_factor():
        yield from needs(("y3", 0), ("y3", 1))
        for c in range(2):
            full[0, :, lanes_at(256 * me.core + 128 * c, 128)] = rows[1, c, rows_at(block * 128, 128), :]
        yield from swap_slab(0)
        local[0] = exact(full[0], full[0, :, half], ((0,), (0,))) / 8192
        yield from all_sum(0, inverse.at[0])
        for k in range(0, 8, 2):
            factor_blocks(inverse.at[0], k, k + 2)
            yield
        lower_only(inverse.at[0])
        done.add("first")

    def second_factor():
        yield from needs(("v3", 0), ("v3", 1))
        for c in range(2):
            full[1, :, lanes_at(256 * me.core + 128 * c, 128)] = cols[3, c, rows_at(me.x * 128, 128), :]
        yield from swap_slab(1)
        yield from needs("first")
        mapped[0] = exact(full[1], inverse[0], ((1,), (1,)))
        local[1] = exact(mapped[0], mapped[0, :, half], ((0,), (0,))) / 8192
        done.add("filtered")
        yield from all_sum(1, inverse.at[1])
        for k in range(0, 8, 2):
            factor_blocks(inverse.at[1], k, k + 2)
            yield
        lower_only(inverse.at[1])
        done.add("second")

    def cross_terms():
        yield from needs(("z2", 0), ("z2", 1), "filtered")
        yield from swap_slab(2)
        mapped[1] = exact(full[2], inverse[0], ((1,), (1,)))
        local[2] = exact(mapped[0], mapped[1, :, half], ((0,), (0,))) / 8192
        yield from all_sum(2, cross)

    live = [chain(0), chain(1), first_factor(), second_factor(), cross_terms()]
    while live:
        for one in list(live):
            if next(one, "end") == "end":
                live.remove(one)

    mine = rows_at(64 * me.core, 64)
    basis = exact(mapped[0, mine, :], inverse[1], ((1,), (1,)))
    basis_out[...] = basis
    cross[...] = exact(inverse[1], cross[...])
    proj_out[...] = exact(cross[...], inverse[1], ((1,), (1,)))
    resid_out[...] = exact(mapped[1, mine, :], inverse[1], ((1,), (1,))) - exact(basis, proj_out[...])


def chain_call(matrix, slab, interval):
    vm = pl.BlockSpec(memory_space=pltpu.VMEM)
    dma = pltpu.SemaphoreType.DMA
    slab_shape = jax.ShapeDtypeStruct((64, 512), F32)
    return pl.pallas_call(
        chain_kernel,
        out_shape=(slab_shape, jax.ShapeDtypeStruct((512, 512), F32), slab_shape),
        in_specs=[pl.BlockSpec(memory_space=pltpu.SMEM), vm, vm],
        out_specs=(vm, vm, vm),
        scratch_shapes=[
            pltpu.VMEM((1024, 512), F32),
            pltpu.VMEM((2048, 512), BF16),
            pltpu.VMEM((2048, 512), BF16),
            pltpu.VMEM((512, 2048), BF16),
            pltpu.VMEM((512, 2048), BF16),
            pltpu.VMEM((4, 2, 512, 128), F32),
            pltpu.VMEM((3, 2, 2048, 128), F32),
            pltpu.VMEM((2, 2048, 128), F32),
            pltpu.VMEM((2, 512, 256), BF16),
            pltpu.VMEM((2, 2048, 256), BF16),
            pltpu.VMEM((4, 2, 4, 256, 128), F32),
            pltpu.VMEM((2, 4, 256, 128), F32),
            pltpu.VMEM((4, 2, 4, 128, 128), F32),
            pltpu.VMEM((2, 4, 128, 128), F32),
            pltpu.VMEM((4, 2, 4, 128, 128), F32),
            pltpu.VMEM((2, 4, 128, 128), F32),
            pltpu.VMEM((4, 2, 4, 128, 128), F32),
            pltpu.VMEM((2, 4, 128, 128), F32),
            pltpu.VMEM((2, 512, 128), F32),
            pltpu.VMEM((3, 2, 512, 128), F32),
            pltpu.VMEM((2, 512, 128), F32),
            pltpu.VMEM((3, 2, 512, 128), F32),
            pltpu.VMEM((3, 128, 512), F32),
            pltpu.VMEM((2, 128, 512), F32),
            pltpu.VMEM((3, 512, 256), F32),
            pltpu.VMEM((3, 512, 256), F32),
            pltpu.VMEM((2, 5, 6, 48, 256), F32),
            pltpu.VMEM((3, 6, 6, 48, 256), F32),
            pltpu.VMEM((2, 512, 512), F32),
            pltpu.VMEM((512, 512), F32),
            dma((4, 2, 4, 6)),
            dma((4, 2, 4, 6)),
            dma((3, 2, 2, 2)),
            dma((3, 2, 2, 2)),
            dma((8, 2)),
            dma((8, 2)),
            dma,
            dma,
            dma((2, 4)),
            dma((2, 4)),
            dma((3,)),
            dma((3,)),
            dma((3, 6, 7)),
            dma((3, 6, 7)),
            dma((3,)),
            dma((3,)),
        ],
        compiler_params=pltpu.CompilerParams(has_side_effects=True, collective_id=0, vmem_limit_bytes=VMEM_LIMIT),
    )(interval, matrix, slab)


def shards(matrix, start_vectors, interval):
    return chain_call(matrix, start_vectors, interval)


def solution(mesh):
    torus = Mesh(mesh.devices.reshape(4, 2, 4, 4), ("row_0", "row_1", "col_0", "col_1"))
    placed = (P(ROW, COL), P(COL_ROW, None), P())
    return jax.shard_map(
        shards,
        mesh=torus,
        in_specs=placed,
        out_specs=(P(COL_ROW, None), P(), P(COL_ROW, None)),
        check_vma=False,
    )
```

```python
import jax
import jax.numpy as jnp
from jax import lax
from jax.experimental import pallas as pl
from jax.experimental.pallas import tpu as pltpu
from jax.sharding import Mesh
from jax.sharding import PartitionSpec as P

ROW = ("row_0", "row_1")
COL = ("col_0", "col_1")
COL_ROW = ("col_0", "col_1", "row_0", "row_1")
MESH = pl.DeviceIdType.MESH
F32 = jnp.float32
BF16 = jnp.bfloat16
AXES6 = ("xa", "xb", "ya", "yb", "za", "zb"), ("xb", "xa", "yb", "ya", "zb", "za")
SUM_LINKS = tuple(order[k:] + order[:k] for k in (0, 2, 4) for order in AXES6)
SUM_HALF = 48, 48, 40, 40, 40, 40
SUM_START = 0, 96, 192, 272, 352, 432
VMEM_LIMIT = 63 * 1024 * 1024
LINKS = ("ya", "yb", "za", "zb"), ("yb", "ya", "zb", "za"), ("za", "zb", "ya", "yb"), ("zb", "za", "yb", "ya")


class Place:
    def __init__(self):
        self.x = lax.axis_index("row_0")
        self.core = lax.axis_index("row_1")
        self.z = lax.axis_index("col_0")
        self.y = lax.axis_index("col_1")
        self.at = {"x": self.x, "y": self.y, "z": self.z}

    def device(self, x=None, core=None, z=None, y=None):
        pick = lambda given, own: own if given is None else given
        return (pick(x, self.x), pick(core, self.core), pick(z, self.z), pick(y, self.y))

    def sibling(self):
        return self.device(core=1 - self.core)

    def partner(self, link):
        v = self.at[link[0]]
        w = v + 1 - 2 * (v % 2) if link[1] == "a" else 3 - v
        return self.device(**{link[0]: w})

    def bit(self, link):
        v = self.at[link[0]]
        return ((v + 1) // 2) % 2 if link[1] == "a" else v // 2


def remote(src, dst, send, recv, device):
    return pltpu.make_async_remote_copy(
        src_ref=src, dst_ref=dst, send_sem=send, recv_sem=recv, device_id=device, device_id_type=MESH
    )


def rows_at(start, size):
    return pl.ds(pl.multiple_of(start, size), size)


def chosen(index, values):
    result = values[-1]
    for i, value in list(enumerate(values))[-2::-1]:
        result = jnp.where(index == i, value, result)
    return result


def lanes_at(start, size):
    return pl.ds(pl.multiple_of(start, 128), size)


def halves(value):
    hi = value.astype(BF16)
    return hi, (value - hi.astype(F32)).astype(BF16)


def dot(left, right):
    return jnp.dot(left, right, preferred_element_type=F32)


def thirds(value):
    a = value.astype(BF16)
    rest = value - a.astype(F32)
    b = rest.astype(BF16)
    return a, b, (rest - b.astype(F32)).astype(BF16)


def small_factor(tile):
    sub = lax.broadcasted_iota(jnp.int32, (8, 128), 0)
    w = [tile[8 * i : 8 * i + 8, :] for i in range(8)]
    for p in range(8):
        col = {(i, c): jnp.broadcast_to(w[i][:, 8 * p + c : 8 * p + c + 1], (8, 128)) for i in range(p, 8) for c in range(8)}
        for c in range(8):
            inv = lax.rsqrt(jnp.broadcast_to(col[p, c][c : c + 1, :], (8, 128)))
            row = jnp.broadcast_to(w[p][c : c + 1, :], (8, 128)) * inv
            own = col[p, c] * inv
            below = sub > c
            w[p] = jnp.where(below, w[p] - own * row, jnp.where(sub == c, row, w[p]))
            steps = [jnp.broadcast_to(col[p, c][d : d + 1, :], (8, 128)) * inv for d in range(c + 1, 8)]
            for d in range(c + 1, 8):
                col[p, d] = col[p, d] - own * steps[d - c - 1]
            for i in range(p + 1, 8):
                mult = col[i, c] * inv
                w[i] = w[i] - mult * row
                for d in range(c + 1, 8):
                    col[i, d] = col[i, d] - mult * steps[d - c - 1]
    return jnp.concatenate(w, axis=0)


def factor_blocks(x, first, last):
    def block(k, carry):
        here = pl.ds(pl.multiple_of(64 * k, 64), 64)
        pair = pl.ds(pl.multiple_of(128 * (k // 2), 128), 128)
        odd = k % 2
        lane = lax.broadcasted_iota(jnp.int32, (64, 128), 1)
        rowi = lax.broadcasted_iota(jnp.int32, (64, 128), 0)
        a = x[here, pair]
        a = jnp.where(odd == 1, pltpu.roll(a, 64, 1), a)
        w = small_factor(jnp.where(lane < 64, a, (lane - 64 == rowi).astype(F32)))
        linv = pltpu.roll(w, 64, 1)[:, :64]
        rows = jnp.dot(linv, x[here, :], precision=lax.Precision.HIGHEST, preferred_element_type=F32)
        x[here, :] = rows
        placed = jnp.where(odd == 1, w, pltpu.roll(w, 64, 1))
        x[here, pair] = jnp.where(lane // 64 == odd, placed, x[here, pair])
        full = x[here, :]
        wide = lax.broadcasted_iota(jnp.int32, (64, 512), 1)
        left = jnp.where(wide // 64 > k, full, 0.0)
        h, m, l = thirds(full)
        lh, lm, ll = thirds(left)
        right = jnp.concatenate([h, m, h, m, l, h], axis=0)
        lefts = jnp.concatenate([lh, lh, lm, lm, lh, ll], axis=0)
        update = lax.dot_general(lefts, right, (((0,), (0,)), ((), ())), preferred_element_type=F32)
        r = lax.broadcasted_iota(jnp.int32, (512, 512), 0)
        c = lax.broadcasted_iota(jnp.int32, (512, 512), 1)
        x[...] = jnp.where((c // 64 == k) & (r // 64 > k), 0.0, x[...]) - update
        return carry

    lax.fori_loop(first, last, block, 0)


def lower_only(x):
    for i in range(4):
        strip = pl.ds(128 * i, 128)
        r = 128 * i + lax.broadcasted_iota(jnp.int32, (128, 512), 0)
        c = lax.broadcasted_iota(jnp.int32, (128, 512), 1)
        x[strip, :] = jnp.where(c <= r, x[strip, :], 0.0)


def precise(lefts, rights):
    (a, b, c), (x, y, z) = lefts, rights
    return (dot(b, y) + dot(a, z) + dot(c, x)) + (dot(a, y) + dot(b, x)) + dot(a, x)


def precise_gram(lefts, rights):
    (a, b, c), (x, y, z) = lefts, rights
    tall = jnp.concatenate([a, a, b, b, a, c], axis=0)
    other = jnp.concatenate([x, y, x, y, z, x], axis=0)
    return lax.dot_general(tall, other, (((0,), (0,)), ((), ())), preferred_element_type=F32)


def chain_kernel(
    interval, matrix, slab, basis_out, proj_out, resid_out,
    other, m_hi, m_lo, t_hi, t_lo, cols, rows, part, split_c, split_r,
    r1, h1, r2, h2, r3, h3, r4, share,
    tb, rb1, tb2, rb2, full, mapped, local, total, term, got, inverse, cross, turned, parts,
    f_send, f_recv, b_send, b_recv, g_send, g_recv, m_send, m_recv, p_send, p_recv, s_send, s_recv,
    a_send, a_recv, x_send, x_recv,
):
    me = Place()
    block = me.z * 4 + me.y

    barrier = pltpu.get_barrier_semaphore()
    near = [me.device(x=(me.x + d // 2) % 4, core=(me.core + d) % 2) for d in range(1, 8)]
    near += [me.partner(link) for link in ("ya", "yb", "za", "zb")]
    for device in near:
        pl.semaphore_signal(barrier, inc=1, device_id=device, device_id_type=MESH)
    pl.semaphore_wait(barrier, len(near))

    swap = remote(matrix, other, m_send, m_recv, me.sibling())
    swap.start()

    def slab_rows(x, core):
        return rows_at((x * 2 + core) * 64, 64)

    gathers = []
    for d in range(1, 8):
        to_x, to_core = (me.x + d // 2) % 4, (me.core + d) % 2
        for c in range(2):
            copy = remote(
                slab.at[:, lanes_at(256 * to_core + 128 * c, 128)], cols.at[0, c, slab_rows(me.x, me.core)],
                g_send.at[d, c], g_recv.at[d, c], me.device(x=to_x, core=to_core),
            )
            copy.start()
            gathers.append((d, c, copy))
    for c in range(2):
        cols[0, c, slab_rows(me.x, me.core), :] = slab[:, lanes_at(256 * me.core + 128 * c, 128)]

    center = 0.5 * (interval[0] + interval[1])
    half_width = 0.5 * (interval[1] - interval[0])

    def prepare(source, half):
        def tile(i, carry):
            base = half * 1024 + i * 256
            value = source[rows_at(i * 256, 256), :]
            row = me.x * 2048 + base + lax.broadcasted_iota(jnp.int32, (256, 512), 0)
            col = block * 512 + lax.broadcasted_iota(jnp.int32, (256, 512), 1)
            value = jnp.where(row == col, value - center, value) / half_width
            hi, lo = halves(value)
            where = rows_at(base, 256)
            m_hi[where, :] = hi
            m_lo[where, :] = lo
            hi, lo = halves(value.T)
            t_hi[:, where] = hi
            t_lo[:, where] = lo
            return carry

        lax.fori_loop(0, 4, tile, 0)

    prepare(matrix, me.core)
    swap.wait()
    prepare(other, 1 - me.core)
    for d, c, copy in gathers:
        copy.wait()

    def forward(c, f, source, target, before, last=False):
        hi, lo = halves(cols[source, c])
        split_c[c, :, :128] = hi
        split_c[c, :, 128:] = lo
        copies = {}

        def send(q, step, src, dst, link):
            copies[q, step] = remote(src, dst, f_send.at[f, c, q, step], f_recv.at[f, c, q, step], me.partner(link))
            copies[q, step].start()

        links = [order[0] for order in LINKS]

        def multiply(q, carry):
            strip = rows_at(512 * q, 512)
            both = split_c[c]
            product = dot(m_hi[strip, :], both) + dot(m_lo[strip, :], both)
            part[c, strip, :] = product[:, :128] + product[:, 128:]
            k1 = chosen(q, [me.bit(link) for link in links])
            there = [chosen(q, [me.partner(link)[i] for link in links]) for i in range(4)]
            remote(
                part.at[c, rows_at(512 * q + 256 * (1 - k1), 256)], r1.at[f, c, q],
                f_send.at[f, c, q, 0], f_recv.at[f, c, q, 0], tuple(there),
            ).start()
            return carry

        lax.fori_loop(0, 4, multiply, 0)
        where1, where2 = [], []
        for q, (l1, l2, l3, l4) in enumerate(LINKS):
            k1, k2 = me.bit(l1), me.bit(l2)
            where1.append(512 * q + 256 * k1)
            where2.append(512 * q + 256 * k1 + 128 * k2)
            copies[q, 0] = remote(
                part.at[c, rows_at(512 * q + 256 * (1 - k1), 256)], r1.at[f, c, q],
                f_send.at[f, c, q, 0], f_recv.at[f, c, q, 0], me.partner(l1),
            )
        yield
        for q, (l1, l2, l3, l4) in enumerate(LINKS):
            k2 = me.bit(l2)
            copies[q, 0].wait_recv()
            h1[c, q] = part[c, rows_at(where1[q], 256), :] + r1[f, c, q]
            send(q, 1, h1.at[c, q, rows_at(128 * (1 - k2), 128)], r2.at[f, c, q], l2)
        yield
        for q, (l1, l2, l3, l4) in enumerate(LINKS):
            k2 = me.bit(l2)
            copies[q, 1].wait_recv()
            h2[c, q] = h1[c, q, rows_at(128 * k2, 128), :] + r2[f, c, q]
            if not last:
                send(q, 2, h2.at[c, q], r3.at[f, c, q], l3)
        if last:
            for copy in copies.values():
                copy.wait_send()
            return
        yield
        for q, (l1, l2, l3, l4) in enumerate(LINKS):
            copies[q, 2].wait_recv()
            h3[c, q] = h2[c, q] + r3[f, c, q]
            send(q, 3, h3.at[c, q], r4.at[f, c, q], l4)
        yield
        for q, (l1, l2, l3, l4) in enumerate(LINKS):
            copies[q, 3].wait_recv()
            total = h3[c, q] + r4[f, c, q]
            here = rows_at(where2[q], 128)
            if before is not None:
                total = 2.0 * total - rows[before, c, here, :]
            rows[target, c, here, :] = total
            send(q, 4, rows.at[target, c, here], rows.at[target, c, here], l2)
        yield
        for q, (l1, l2, l3, l4) in enumerate(LINKS):
            copies[q, 4].wait_recv()
            here = rows_at(where1[q], 256)
            send(q, 5, rows.at[target, c, here], rows.at[target, c, here], l1)
        yield
        for q in range(4):
            copies[q, 5].wait_recv()
        for copy in copies.values():
            copy.wait_send()

    def backward(c, b, source, target, before):
        def split(i, carry):
            strip = rows_at(512 * i, 512)
            hi, lo = halves(rows[source, c, strip, :])
            split_r[c, strip, :128] = hi
            split_r[c, strip, 128:] = lo
            return carry

        lax.fori_loop(0, 4, split, 0)
        orders = ("xa", "xb"), ("xb", "xa")
        copies = {}

        def send(s, step, src, dst, link):
            copies[s, step] = remote(src, dst, b_send.at[b, c, s, step], b_recv.at[b, c, s, step], me.partner(link))
            copies[s, step].start()

        def multiply(s, carry):
            strip = rows_at(256 * s, 256)
            both = split_r[c]
            product = dot(t_hi[strip, :], both) + dot(t_lo[strip, :], both)
            tb[c, strip, :] = product[:, :128] + product[:, 128:]
            there = [chosen(s, [me.partner(order[0])[i] for order in orders]) for i in range(4)]
            remote(
                tb.at[c, strip], rb1.at[b, c, strip], b_send.at[b, c, s, 0], b_recv.at[b, c, s, 0], tuple(there)
            ).start()
            return carry

        lax.fori_loop(0, 2, multiply, 0)
        for s in range(2):
            strip = pl.ds(256 * s, 256)
            copies[s, 0] = remote(
                tb.at[c, strip], rb1.at[b, c, strip],
                b_send.at[b, c, s, 0], b_recv.at[b, c, s, 0], me.partner(orders[s][0]),
            )
        yield
        for s in range(2):
            strip = pl.ds(256 * s, 256)
            copies[s, 0].wait_recv()
            tb2[c, strip, :] = tb[c, strip, :] + rb1[b, c, strip, :]
            send(s, 1, tb2.at[c, strip], rb2.at[b, c, strip], orders[s][1])
        yield
        for s in range(2):
            strip = pl.ds(256 * s, 256)
            copies[s, 1].wait_recv()
            total = tb2[c, strip, :] + rb2[b, c, strip, :]
            if before is not None:
                total = 2.0 * total - cols[before, c, strip, :]
            cols[target, c, strip, :] = total
        for copy in copies.values():
            copy.wait_send()

    done = set()

    def chain(c):
        yield from forward(c, 0, 0, 0, None)
        yield from backward(c, 0, 0, 1, 0)
        yield from forward(c, 1, 1, 1, 0)
        done.add(("y3", c))
        yield from backward(c, 1, 1, 2, None)
        yield from forward(c, 2, 2, 2, 1)
        yield from backward(c, 2, 2, 3, 2)
        done.add(("v3", c))
        yield from forward(c, 3, 3, None, None, last=True)
        mine = lanes_at(256 * me.core + 128 * c, 128)
        pending = []
        own_index = None
        for q, (l1, l2, l3, l4) in enumerate(LINKS):
            k1, k2, k3, k4 = me.bit(l1), me.bit(l2), me.bit(l3), me.bit(l4)
            to_x, to_y, to_z = 2 * k1 + k2, q, me.x
            index = 2 * k3 + k4
            same = (to_x == me.x) & (to_y == me.y) & (to_z == me.z)
            own_index = jnp.where(same, index, -1 if own_index is None else own_index)
            copy = remote(
                h2.at[c, q], share.at[c, index],
                p_send.at[c, q], p_recv.at[c, index], me.device(x=to_x, y=to_y, z=to_z),
            )

            @pl.when(jnp.logical_not(same))
            def _():
                copy.start()

            @pl.when(same)
            def _():
                share[c, index] = h2[c, q]

            pending.append((same, copy))
        yield
        for same, copy in pending:

            @pl.when(jnp.logical_not(same))
            def _():
                copy.wait_send()

        for index in range(4):

            @pl.when(own_index != index)
            def _():
                remote(
                    h2.at[c, 0], share.at[c, index], p_send.at[c, 0], p_recv.at[c, index], me.sibling()
                ).wait_recv()

        full[2, :, mine] = (share[c, 0] + share[c, 1]) + (share[c, 2] + share[c, 3])
        done.add(("z2", c))

    half = lanes_at(256 * me.core, 256)

    def needs(*marks):
        while not all(mark in done for mark in marks):
            yield "blocked"

    def swap_slab(k):
        copy = remote(full.at[k, :, half], full.at[k, :, half], s_send.at[k], s_recv.at[k], me.sibling())
        copy.start()
        yield
        copy.wait()

    def all_sum(n, target):
        copies = {}

        def send(s, t, src, dst, link):
            copies[s, t] = remote(src, dst, a_send.at[n, s, t], a_recv.at[n, s, t], me.partner(link))
            copies[s, t].start()

        def piece(s, k):
            return pl.ds(pl.multiple_of(SUM_START[s] + SUM_HALF[s] * k, 8), SUM_HALF[s])

        for s, order in enumerate(SUM_LINKS):
            small = pl.ds(0, SUM_HALF[s])
            send(s, 0, local.at[n, piece(s, 1 - me.bit(order[0]))], got.at[n, 0, s, small], order[0])
        yield
        for t in range(1, 6):
            for s, order in enumerate(SUM_LINKS):
                small = pl.ds(0, SUM_HALF[s])
                copies[s, t - 1].wait_recv()
                before = local[n, piece(s, me.bit(order[0])), :] if t == 1 else term[n % 2, t - 2, s, small, :]
                term[n % 2, t - 1, s, small, :] = before + got[n, t - 1, s, small, :]
                send(s, t, term.at[n % 2, t - 1, s, small], got.at[n, t, s, small], order[t])
            yield
        for s, order in enumerate(SUM_LINKS):
            small = pl.ds(0, SUM_HALF[s])
            copies[s, 5].wait_recv()
            here = piece(s, me.bit(order[0]))
            total[n, here, :] = term[n % 2, 4, s, small, :] + got[n, 5, s, small, :]
            send(s, 6, total.at[n, here], total.at[n, here], order[0])
        yield
        for s in range(6):
            copies[s, 6].wait_recv()
        copy = remote(total.at[n], target.at[:, half], x_send.at[n], x_recv.at[n], me.sibling())
        copy.start()
        target[:, half] = total[n]
        for one in copies.values():
            one.wait_send()
        yield
        copy.wait()

    def keep_transposed(x):
        for i, one in enumerate(thirds(x[...].T)):
            turned[i] = one

    def transposed():
        return turned[0], turned[1], turned[2]

    def first_factor():
        yield from needs(("y3", 0), ("y3", 1))
        for c in range(2):
            full[0, :, lanes_at(256 * me.core + 128 * c, 128)] = rows[1, c, rows_at(block * 128, 128), :]
        yield from swap_slab(0)
        local[0] = precise_gram(thirds(full[0]), thirds(full[0, :, half])) / 8192
        yield from all_sum(0, inverse.at[0])
        for k in range(0, 8, 2):
            factor_blocks(inverse.at[0], k, k + 2)
            yield
        lower_only(inverse.at[0])
        keep_transposed(inverse.at[0])
        done.add("first")

    def second_factor():
        yield from needs(("v3", 0), ("v3", 1))
        for c in range(2):
            full[1, :, lanes_at(256 * me.core + 128 * c, 128)] = cols[3, c, rows_at(me.x * 128, 128), :]
        yield from swap_slab(1)
        yield from needs("first")
        mapped[0] = precise(thirds(full[1]), transposed())
        local[1] = precise_gram(thirds(mapped[0]), thirds(mapped[0, :, half])) / 8192
        done.add("filtered")
        yield from all_sum(1, inverse.at[1])
        for k in range(0, 8, 2):
            factor_blocks(inverse.at[1], k, k + 2)
            yield
        lower_only(inverse.at[1])
        done.add("second")

    def cross_terms():
        yield from needs(("z2", 0), ("z2", 1), "filtered")
        yield from swap_slab(2)
        mapped[1] = precise(thirds(full[2]), transposed())
        local[2] = precise_gram(thirds(mapped[0]), thirds(mapped[1, :, half])) / 8192
        yield from all_sum(2, cross)

    live = [chain(0), chain(1), first_factor(), second_factor(), cross_terms()]
    while live:
        for one in list(live):
            if next(one, "end") == "end":
                live.remove(one)

    keep_transposed(inverse.at[1])
    mine = rows_at(64 * me.core, 64)
    basis = precise(thirds(mapped[0, mine, :]), transposed())
    basis_out[...] = basis
    for i, one in enumerate(thirds(cross[...])):
        parts[i] = one

    def solve_left(i, carry):
        strip = rows_at(256 * i, 256)
        cross[strip, :] = precise(thirds(inverse[1, strip, :]), (parts[0], parts[1], parts[2]))
        return carry

    lax.fori_loop(0, 2, solve_left, 0)

    def solve_right(i, carry):
        strip = rows_at(256 * i, 256)
        proj_out[strip, :] = precise(thirds(cross[strip, :]), transposed())
        return carry

    lax.fori_loop(0, 2, solve_right, 0)
    rest = mapped[1, mine, :] - precise(thirds(basis), thirds(cross[...]))
    resid_out[...] = precise(thirds(rest), transposed())


def chain_call(matrix, slab, interval):
    vm = pl.BlockSpec(memory_space=pltpu.VMEM)
    dma = pltpu.SemaphoreType.DMA
    slab_shape = jax.ShapeDtypeStruct((64, 512), F32)
    return pl.pallas_call(
        chain_kernel,
        out_shape=(slab_shape, jax.ShapeDtypeStruct((512, 512), F32), slab_shape),
        in_specs=[pl.BlockSpec(memory_space=pltpu.SMEM), vm, vm],
        out_specs=(vm, vm, vm),
        scratch_shapes=[
            pltpu.VMEM((1024, 512), F32),
            pltpu.VMEM((2048, 512), BF16),
            pltpu.VMEM((2048, 512), BF16),
            pltpu.VMEM((512, 2048), BF16),
            pltpu.VMEM((512, 2048), BF16),
            pltpu.VMEM((4, 2, 512, 128), F32),
            pltpu.VMEM((3, 2, 2048, 128), F32),
            pltpu.VMEM((2, 2048, 128), F32),
            pltpu.VMEM((2, 512, 256), BF16),
            pltpu.VMEM((2, 2048, 256), BF16),
            pltpu.VMEM((4, 2, 4, 256, 128), F32),
            pltpu.VMEM((2, 4, 256, 128), F32),
            pltpu.VMEM((4, 2, 4, 128, 128), F32),
            pltpu.VMEM((2, 4, 128, 128), F32),
            pltpu.VMEM((3, 2, 4, 128, 128), F32),
            pltpu.VMEM((2, 4, 128, 128), F32),
            pltpu.VMEM((3, 2, 4, 128, 128), F32),
            pltpu.VMEM((2, 4, 128, 128), F32),
            pltpu.VMEM((2, 512, 128), F32),
            pltpu.VMEM((3, 2, 512, 128), F32),
            pltpu.VMEM((2, 512, 128), F32),
            pltpu.VMEM((3, 2, 512, 128), F32),
            pltpu.VMEM((3, 128, 512), F32),
            pltpu.VMEM((2, 128, 512), F32),
            pltpu.VMEM((3, 512, 256), F32),
            pltpu.VMEM((3, 512, 256), F32),
            pltpu.VMEM((2, 5, 6, 48, 256), F32),
            pltpu.VMEM((3, 6, 6, 48, 256), F32),
            pltpu.VMEM((2, 512, 512), F32),
            pltpu.VMEM((512, 512), F32),
            pltpu.VMEM((3, 512, 512), BF16),
            pltpu.VMEM((3, 512, 512), BF16),
            dma((4, 2, 4, 6)),
            dma((4, 2, 4, 6)),
            dma((3, 2, 2, 2)),
            dma((3, 2, 2, 2)),
            dma((8, 2)),
            dma((8, 2)),
            dma,
            dma,
            dma((2, 4)),
            dma((2, 4)),
            dma((3,)),
            dma((3,)),
            dma((3, 6, 7)),
            dma((3, 6, 7)),
            dma((3,)),
            dma((3,)),
        ],
        compiler_params=pltpu.CompilerParams(has_side_effects=True, collective_id=0, vmem_limit_bytes=VMEM_LIMIT),
    )(interval, matrix, slab)


def shards(matrix, start_vectors, interval):
    return chain_call(matrix, start_vectors, interval)


def solution(mesh):
    torus = Mesh(mesh.devices.reshape(4, 2, 4, 4), ("row_0", "row_1", "col_0", "col_1"))
    placed = (P(ROW, COL), P(COL_ROW, None), P())
    return jax.shard_map(
        shards,
        mesh=torus,
        in_specs=placed,
        out_specs=(P(COL_ROW, None), P(), P(COL_ROW, None)),
        check_vma=False,
    )
```

```python
import jax
import jax.numpy as jnp
from jax import lax
from jax.experimental import pallas as pl
from jax.experimental.pallas import tpu as pltpu
from jax.sharding import Mesh
from jax.sharding import PartitionSpec as P

ROW = ("row_0", "row_1")
COL = ("col_0", "col_1")
COL_ROW = ("col_0", "col_1", "row_0", "row_1")
MESH = pl.DeviceIdType.MESH
F32 = jnp.float32
BF16 = jnp.bfloat16
AXES6 = ("xa", "xb", "ya", "yb", "za", "zb"), ("xb", "xa", "yb", "ya", "zb", "za")
SUM_LINKS = tuple(order[k:] + order[:k] for k in (0, 2, 4) for order in AXES6)
SUM_HALF = 48, 48, 40, 40, 40, 40
SUM_START = 0, 96, 192, 272, 352, 432
VMEM_LIMIT = 63 * 1024 * 1024
LINKS = ("ya", "yb", "za", "zb"), ("yb", "ya", "zb", "za"), ("za", "zb", "ya", "yb"), ("zb", "za", "yb", "ya")
STREAMS = LINKS + LINKS


class Place:
    def __init__(self):
        self.x = lax.axis_index("row_0")
        self.core = lax.axis_index("row_1")
        self.z = lax.axis_index("col_0")
        self.y = lax.axis_index("col_1")
        self.at = {"x": self.x, "y": self.y, "z": self.z}

    def device(self, x=None, core=None, z=None, y=None):
        pick = lambda given, own: own if given is None else given
        return (pick(x, self.x), pick(core, self.core), pick(z, self.z), pick(y, self.y))

    def sibling(self):
        return self.device(core=1 - self.core)

    def partner(self, link):
        v = self.at[link[0]]
        w = v + 1 - 2 * (v % 2) if link[1] == "a" else 3 - v
        return self.device(**{link[0]: w})

    def bit(self, link):
        v = self.at[link[0]]
        return ((v + 1) // 2) % 2 if link[1] == "a" else v // 2


def remote(src, dst, send, recv, device):
    return pltpu.make_async_remote_copy(
        src_ref=src, dst_ref=dst, send_sem=send, recv_sem=recv, device_id=device, device_id_type=MESH
    )


def rows_at(start, size):
    return pl.ds(pl.multiple_of(start, size), size)


def chosen(index, values):
    result = values[-1]
    for i, value in list(enumerate(values))[-2::-1]:
        result = jnp.where(index == i, value, result)
    return result


def lanes_at(start, size):
    return pl.ds(pl.multiple_of(start, 128), size)


def halves(value):
    hi = value.astype(BF16)
    return hi, (value - hi.astype(F32)).astype(BF16)


def dot(left, right):
    return jnp.dot(left, right, preferred_element_type=F32)


def thirds(value):
    a = value.astype(BF16)
    rest = value - a.astype(F32)
    b = rest.astype(BF16)
    return a, b, (rest - b.astype(F32)).astype(BF16)


def small_factor(tile):
    sub = lax.broadcasted_iota(jnp.int32, (8, 128), 0)
    w = [tile[8 * i : 8 * i + 8, :] for i in range(8)]
    for p in range(8):
        col = {(i, c): jnp.broadcast_to(w[i][:, 8 * p + c : 8 * p + c + 1], (8, 128)) for i in range(p, 8) for c in range(8)}
        for c in range(8):
            inv = lax.rsqrt(jnp.broadcast_to(col[p, c][c : c + 1, :], (8, 128)))
            row = jnp.broadcast_to(w[p][c : c + 1, :], (8, 128)) * inv
            own = col[p, c] * inv
            below = sub > c
            w[p] = jnp.where(below, w[p] - own * row, jnp.where(sub == c, row, w[p]))
            steps = [jnp.broadcast_to(col[p, c][d : d + 1, :], (8, 128)) * inv for d in range(c + 1, 8)]
            for d in range(c + 1, 8):
                col[p, d] = col[p, d] - own * steps[d - c - 1]
            for i in range(p + 1, 8):
                mult = col[i, c] * inv
                w[i] = w[i] - mult * row
                for d in range(c + 1, 8):
                    col[i, d] = col[i, d] - mult * steps[d - c - 1]
    return jnp.concatenate(w, axis=0)


def factor_block(x, k):
    here = pl.ds(pl.multiple_of(64 * k, 64), 64)
    pair = pl.ds(pl.multiple_of(128 * (k // 2), 128), 128)
    odd = k % 2
    lane = lax.broadcasted_iota(jnp.int32, (64, 128), 1)
    rowi = lax.broadcasted_iota(jnp.int32, (64, 128), 0)
    a = x[here, pair]
    a = jnp.where(odd == 1, pltpu.roll(a, 64, 1), a)
    w = small_factor(jnp.where(lane < 64, a, (lane - 64 == rowi).astype(F32)))
    linv = pltpu.roll(w, 64, 1)[:, :64]
    rows = jnp.dot(linv, x[here, :], precision=lax.Precision.HIGHEST, preferred_element_type=F32)
    x[here, :] = rows
    placed = jnp.where(odd == 1, w, pltpu.roll(w, 64, 1))
    x[here, pair] = jnp.where(lane // 64 == odd, placed, x[here, pair])
    full = x[here, :]
    wide = lax.broadcasted_iota(jnp.int32, (64, 512), 1)
    left = jnp.where(wide // 64 > k, full, 0.0)
    h, m, l = thirds(full)
    lh, lm, ll = thirds(left)
    right = jnp.concatenate([h, m, h, m, l, h], axis=0)
    lefts = jnp.concatenate([lh, lh, lm, lm, lh, ll], axis=0)
    update = lax.dot_general(lefts, right, (((0,), (0,)), ((), ())), preferred_element_type=F32)
    r = lax.broadcasted_iota(jnp.int32, (512, 512), 0)
    c = lax.broadcasted_iota(jnp.int32, (512, 512), 1)
    x[...] = jnp.where((c // 64 == k) & (r // 64 > k), 0.0, x[...]) - update


def lower_only(x):
    for i in range(4):
        strip = pl.ds(128 * i, 128)
        r = 128 * i + lax.broadcasted_iota(jnp.int32, (128, 512), 0)
        c = lax.broadcasted_iota(jnp.int32, (128, 512), 1)
        x[strip, :] = jnp.where(c <= r, x[strip, :], 0.0)


def precise(lefts, rights):
    (a, b, c), (x, y, z) = lefts, rights
    return (dot(b, y) + dot(a, z) + dot(c, x)) + (dot(a, y) + dot(b, x)) + dot(a, x)


def precise_gram(lefts, rights):
    (a, b, c), (x, y, z) = lefts, rights
    tall = jnp.concatenate([a, a, b, b, a, c], axis=0)
    other = jnp.concatenate([x, y, x, y, z, x], axis=0)
    return lax.dot_general(tall, other, (((0,), (0,)), ((), ())), preferred_element_type=F32)


def chain_kernel(
    interval, matrix, slab, basis_out, proj_out, resid_out,
    other, m_hi, m_lo, t_hi, t_lo, cols, rows, part, split_c, split_r,
    r1, h1, r2, h2, r3, h3, r4, share,
    tb, rb1, tb2, rb2, full, mapped, local, total, term, got, inverse, cross, turned, parts,
    f_send, f_recv, b_send, b_recv, g_send, g_recv, m_send, m_recv, p_send, p_recv, s_send, s_recv,
    a_send, a_recv, x_send, x_recv,
):
    me = Place()
    block = me.z * 4 + me.y

    barrier = pltpu.get_barrier_semaphore()
    near = [me.device(x=(me.x + d // 2) % 4, core=(me.core + d) % 2) for d in range(1, 8)]
    near += [me.partner(link) for link in ("ya", "yb", "za", "zb")]
    for device in near:
        pl.semaphore_signal(barrier, inc=1, device_id=device, device_id_type=MESH)
    pl.semaphore_wait(barrier, len(near))

    swap = remote(matrix, other, m_send, m_recv, me.sibling())
    swap.start()

    def slab_rows(x, core):
        return rows_at((x * 2 + core) * 64, 64)

    gathers = []
    for d in range(1, 8):
        to_x, to_core = (me.x + d // 2) % 4, (me.core + d) % 2
        for c in range(2):
            copy = remote(
                slab.at[:, lanes_at(256 * to_core + 128 * c, 128)], cols.at[0, c, slab_rows(me.x, me.core)],
                g_send.at[d, c], g_recv.at[d, c], me.device(x=to_x, core=to_core),
            )
            copy.start()
            gathers.append((d, c, copy))
    for c in range(2):
        cols[0, c, slab_rows(me.x, me.core), :] = slab[:, lanes_at(256 * me.core + 128 * c, 128)]

    center = 0.5 * (interval[0] + interval[1])
    half_width = 0.5 * (interval[1] - interval[0])

    def prepare(source, half):
        def tile(i, carry):
            base = half * 1024 + i * 256
            value = source[rows_at(i * 256, 256), :]
            row = me.x * 2048 + base + lax.broadcasted_iota(jnp.int32, (256, 512), 0)
            col = block * 512 + lax.broadcasted_iota(jnp.int32, (256, 512), 1)
            value = jnp.where(row == col, value - center, value) / half_width
            hi, lo = halves(value)
            where = rows_at(base, 256)
            m_hi[where, :] = hi
            m_lo[where, :] = lo
            hi, lo = halves(value.T)
            t_hi[:, where] = hi
            t_lo[:, where] = lo
            return carry

        lax.fori_loop(0, 4, tile, 0)

    prepare(matrix, me.core)
    swap.wait()
    prepare(other, 1 - me.core)
    for d, c, copy in gathers:
        copy.wait()

    def forward(c, f, source, target, before, last=False):
        hi, lo = halves(cols[source, c])
        split_c[c, :, :128] = hi
        split_c[c, :, 128:] = lo
        copies = {}

        def send(q, step, src, dst, link):
            copies[q, step] = remote(src, dst, f_send.at[f, c, q, step], f_recv.at[f, c, q, step], me.partner(link))
            copies[q, step].start()

        def multiply(q, carry):
            strip = rows_at(512 * q, 512)
            both = split_c[c]
            product = dot(m_hi[strip, :], both) + dot(m_lo[strip, :], both)
            part[c, strip, :] = product[:, :128] + product[:, 128:]
            for u in range(2):
                links = [STREAMS[2 * i + u][0] for i in range(4)]
                k1 = chosen(q, [me.bit(link) for link in links])
                there = [chosen(q, [me.partner(link)[i] for link in links]) for i in range(4)]
                remote(
                    part.at[c, rows_at(512 * q + 256 * u + 128 * (1 - k1), 128)], r1.at[f, c, 2 * q + u],
                    f_send.at[f, c, 2 * q + u, 0], f_recv.at[f, c, 2 * q + u, 0], tuple(there),
                ).start()
            return carry

        lax.fori_loop(0, 4, multiply, 0)
        where1, where2 = [], []
        for q, (l1, l2, l3, l4) in enumerate(STREAMS):
            k1, k2 = me.bit(l1), me.bit(l2)
            where1.append(256 * q + 128 * k1)
            where2.append(256 * q + 128 * k1 + 64 * k2)
            copies[q, 0] = remote(
                part.at[c, rows_at(256 * q + 128 * (1 - k1), 128)], r1.at[f, c, q],
                f_send.at[f, c, q, 0], f_recv.at[f, c, q, 0], me.partner(l1),
            )
        yield
        for q, (l1, l2, l3, l4) in enumerate(STREAMS):
            k2 = me.bit(l2)
            copies[q, 0].wait_recv()
            h1[c, q] = part[c, rows_at(where1[q], 128), :] + r1[f, c, q]
            send(q, 1, h1.at[c, q, rows_at(64 * (1 - k2), 64)], r2.at[f, c, q], l2)
        yield
        for q, (l1, l2, l3, l4) in enumerate(STREAMS):
            k2 = me.bit(l2)
            copies[q, 1].wait_recv()
            h2[c, q] = h1[c, q, rows_at(64 * k2, 64), :] + r2[f, c, q]
            if not last:
                send(q, 2, h2.at[c, q], r3.at[f, c, q], l3)
        if last:
            for copy in copies.values():
                copy.wait_send()
            return
        yield
        for q, (l1, l2, l3, l4) in enumerate(STREAMS):
            copies[q, 2].wait_recv()
            h3[c, q] = h2[c, q] + r3[f, c, q]
            send(q, 3, h3.at[c, q], r4.at[f, c, q], l4)
        yield
        for q, (l1, l2, l3, l4) in enumerate(STREAMS):
            copies[q, 3].wait_recv()
            total = h3[c, q] + r4[f, c, q]
            here = rows_at(where2[q], 64)
            if before is not None:
                total = 2.0 * total - rows[before, c, here, :]
            rows[target, c, here, :] = total
            send(q, 4, rows.at[target, c, here], rows.at[target, c, here], l2)
        yield
        for q, (l1, l2, l3, l4) in enumerate(STREAMS):
            copies[q, 4].wait_recv()
            here = rows_at(where1[q], 128)
            send(q, 5, rows.at[target, c, here], rows.at[target, c, here], l1)
        yield
        for q in range(8):
            copies[q, 5].wait_recv()
        for copy in copies.values():
            copy.wait_send()

    def backward(c, b, source, target, before):
        def split(i, carry):
            strip = rows_at(512 * i, 512)
            hi, lo = halves(rows[source, c, strip, :])
            split_r[c, strip, :128] = hi
            split_r[c, strip, 128:] = lo
            return carry

        lax.fori_loop(0, 4, split, 0)
        orders = ("xa", "xb"), ("xb", "xa")
        copies = {}

        def send(s, step, src, dst, link):
            copies[s, step] = remote(src, dst, b_send.at[b, c, s, step], b_recv.at[b, c, s, step], me.partner(link))
            copies[s, step].start()

        def multiply(s, carry):
            strip = rows_at(256 * s, 256)
            both = split_r[c]
            product = dot(t_hi[strip, :], both) + dot(t_lo[strip, :], both)
            tb[c, strip, :] = product[:, :128] + product[:, 128:]
            for u in range(2):
                strip = rows_at(256 * s + 128 * u, 128)
                remote(
                    tb.at[c, strip], rb1.at[b, c, strip],
                    b_send.at[b, c, 2 * s + u, 0], b_recv.at[b, c, 2 * s + u, 0], me.partner(orders[u][0]),
                ).start()
            return carry

        lax.fori_loop(0, 2, multiply, 0)
        for s in range(4):
            strip = pl.ds(128 * s, 128)
            copies[s, 0] = remote(
                tb.at[c, strip], rb1.at[b, c, strip],
                b_send.at[b, c, s, 0], b_recv.at[b, c, s, 0], me.partner(orders[s % 2][0]),
            )
        yield
        for s in range(4):
            strip = pl.ds(128 * s, 128)
            copies[s, 0].wait_recv()
            tb2[c, strip, :] = tb[c, strip, :] + rb1[b, c, strip, :]
            send(s, 1, tb2.at[c, strip], rb2.at[b, c, strip], orders[s % 2][1])
        yield
        for s in range(4):
            strip = pl.ds(128 * s, 128)
            copies[s, 1].wait_recv()
            total = tb2[c, strip, :] + rb2[b, c, strip, :]
            if before is not None:
                total = 2.0 * total - cols[before, c, strip, :]
            cols[target, c, strip, :] = total
        for copy in copies.values():
            copy.wait_send()

    done = set()

    def chain(c):
        yield from forward(c, 0, 0, 0, None)
        yield from backward(c, 0, 0, 1, 0)
        yield from forward(c, 1, 1, 1, 0)
        done.add(("y3", c))
        yield from backward(c, 1, 1, 2, None)
        yield from forward(c, 2, 2, 2, 1)
        yield from backward(c, 2, 2, 3, 2)
        done.add(("v3", c))
        yield from forward(c, 3, 3, None, None, last=True)
        mine = lanes_at(256 * me.core + 128 * c, 128)
        pending = []
        own_index = None
        for q, (l1, l2, l3, l4) in enumerate(STREAMS):
            k1, k2, k3, k4 = me.bit(l1), me.bit(l2), me.bit(l3), me.bit(l4)
            to_x, to_y, to_z = 2 * (q % 2) + k1, q // 2, me.x
            index = 2 * k3 + k4
            same = (to_x == me.x) & (to_y == me.y) & (to_z == me.z)
            own_index = jnp.where(same, 4 * k2 + index, -1 if own_index is None else own_index)
            copy = remote(
                h2.at[c, q], share.at[c, k2, index],
                p_send.at[c, q], p_recv.at[c, k2, index], me.device(x=to_x, y=to_y, z=to_z),
            )

            @pl.when(jnp.logical_not(same))
            def _():
                copy.start()

            @pl.when(same)
            def _():
                share[c, k2, index] = h2[c, q]

            pending.append((same, copy))
        yield
        for same, copy in pending:

            @pl.when(jnp.logical_not(same))
            def _():
                copy.wait_send()

        for k2 in range(2):
            for index in range(4):

                @pl.when(own_index != 4 * k2 + index)
                def _():
                    remote(
                        h2.at[c, 0], share.at[c, k2, index], p_send.at[c, 0], p_recv.at[c, k2, index], me.sibling()
                    ).wait_recv()

            pieces = [share[c, k2, index] for index in range(4)]
            full[2, pl.ds(64 * k2, 64), mine] = (pieces[0] + pieces[1]) + (pieces[2] + pieces[3])
        done.add(("z2", c))

    half = lanes_at(256 * me.core, 256)

    def needs(*marks):
        while not all(mark in done for mark in marks):
            yield "blocked"

    def swap_slab(k):
        copy = remote(full.at[k, :, half], full.at[k, :, half], s_send.at[k], s_recv.at[k], me.sibling())
        copy.start()
        yield
        copy.wait()

    def all_sum(n, target):
        def piece(s, k):
            return pl.ds(pl.multiple_of(SUM_START[s] + SUM_HALF[s] * k, 8), SUM_HALF[s])

        small = [pl.ds(0, SUM_HALF[s]) for s in range(6)]
        keep = [piece(s, me.bit(order[0])) for s, order in enumerate(SUM_LINKS)]
        away = [piece(s, 1 - me.bit(order[0])) for s, order in enumerate(SUM_LINKS)]
        copies = {}
        for s, order in enumerate(SUM_LINKS):
            for t in range(7):
                if t == 0:
                    src, dst = local.at[n, away[s]], got.at[n, 0, s, small[s]]
                elif t < 6:
                    src, dst = term.at[n % 2, t - 1, s, small[s]], got.at[n, t, s, small[s]]
                else:
                    src = dst = total.at[n, keep[s]]
                link = order[t % 6]
                copies[s, t] = remote(src, dst, a_send.at[n, s, t], a_recv.at[n, s, t], me.partner(link))
        copy = remote(total.at[n], target.at[:, half], x_send.at[n], x_recv.at[n], me.sibling())
        for s in range(6):
            copies[s, 0].start()
        yield
        for t in range(1, 6):
            for s in range(6):
                copies[s, t - 1].wait_recv()
                before = local[n, keep[s], :] if t == 1 else term[n % 2, t - 2, s, small[s], :]
                term[n % 2, t - 1, s, small[s], :] = before + got[n, t - 1, s, small[s], :]
                copies[s, t].start()
            yield
        for s in range(6):
            copies[s, 5].wait_recv()
            total[n, keep[s], :] = term[n % 2, 4, s, small[s], :] + got[n, 5, s, small[s], :]
            copies[s, 6].start()
        yield
        for s in range(6):
            copies[s, 6].wait_recv()
        copy.start()
        target[:, half] = total[n]
        for one in copies.values():
            one.wait_send()
        yield
        copy.wait()

    def keep_transposed(x):
        for i, one in enumerate(thirds(x[...].T)):
            turned[i] = one

    def transposed():
        return turned[0], turned[1], turned[2]

    def first_factor():
        yield from needs(("y3", 0), ("y3", 1))
        for c in range(2):
            full[0, :, lanes_at(256 * me.core + 128 * c, 128)] = rows[1, c, rows_at(block * 128, 128), :]
        yield from swap_slab(0)
        local[0] = precise_gram(thirds(full[0]), thirds(full[0, :, half])) / 8192
        yield from all_sum(0, inverse.at[0])
        for k in range(8):
            factor_block(inverse.at[0], jnp.int32(k))
            yield
        lower_only(inverse.at[0])
        keep_transposed(inverse.at[0])
        done.add("first")

    def second_factor():
        yield from needs(("v3", 0), ("v3", 1))
        for c in range(2):
            full[1, :, lanes_at(256 * me.core + 128 * c, 128)] = cols[3, c, rows_at(me.x * 128, 128), :]
        yield from swap_slab(1)
        yield from needs("first")
        mapped[0] = precise(thirds(full[1]), transposed())
        local[1] = precise_gram(thirds(mapped[0]), thirds(mapped[0, :, half])) / 8192
        done.add("filtered")
        yield from all_sum(1, inverse.at[1])

    def cross_terms():
        yield from needs(("z2", 0), ("z2", 1), "filtered")
        yield from swap_slab(2)
        mapped[1] = precise(thirds(full[2]), transposed())
        local[2] = precise_gram(thirds(mapped[0]), thirds(mapped[1, :, half])) / 8192
        yield from all_sum(2, cross)

    crossing = cross_terms()
    live = [chain(0), chain(1), first_factor(), second_factor(), crossing]
    while len(live) > 1:
        for one in list(live):
            if next(one, "end") == "end":
                live.remove(one)

    def factor_and_cross(k, carry):
        factor_block(inverse.at[1], k)
        for i in range(8):

            @pl.when(k == i)
            def _():
                next(crossing, "end")

        return carry

    lax.fori_loop(0, 8, factor_and_cross, 0)
    for _ in crossing:
        pass
    lower_only(inverse.at[1])

    keep_transposed(inverse.at[1])
    mine = rows_at(64 * me.core, 64)
    basis = precise(thirds(mapped[0, mine, :]), transposed())
    basis_out[...] = basis
    for i, one in enumerate(thirds(cross[...])):
        parts[i] = one

    def solve_left(i, carry):
        strip = rows_at(256 * i, 256)
        cross[strip, :] = precise(thirds(inverse[1, strip, :]), (parts[0], parts[1], parts[2]))
        return carry

    lax.fori_loop(0, 2, solve_left, 0)

    def solve_right(i, carry):
        strip = rows_at(256 * i, 256)
        proj_out[strip, :] = precise(thirds(cross[strip, :]), transposed())
        return carry

    lax.fori_loop(0, 2, solve_right, 0)
    rest = mapped[1, mine, :] - precise(thirds(basis), thirds(cross[...]))
    resid_out[...] = precise(thirds(rest), transposed())


def chain_call(matrix, slab, interval):
    vm = pl.BlockSpec(memory_space=pltpu.VMEM)
    dma = pltpu.SemaphoreType.DMA
    slab_shape = jax.ShapeDtypeStruct((64, 512), F32)
    return pl.pallas_call(
        chain_kernel,
        out_shape=(slab_shape, jax.ShapeDtypeStruct((512, 512), F32), slab_shape),
        in_specs=[pl.BlockSpec(memory_space=pltpu.SMEM), vm, vm],
        out_specs=(vm, vm, vm),
        scratch_shapes=[
            pltpu.VMEM((1024, 512), F32),
            pltpu.VMEM((2048, 512), BF16),
            pltpu.VMEM((2048, 512), BF16),
            pltpu.VMEM((512, 2048), BF16),
            pltpu.VMEM((512, 2048), BF16),
            pltpu.VMEM((4, 2, 512, 128), F32),
            pltpu.VMEM((3, 2, 2048, 128), F32),
            pltpu.VMEM((2, 2048, 128), F32),
            pltpu.VMEM((2, 512, 256), BF16),
            pltpu.VMEM((2, 2048, 256), BF16),
            pltpu.VMEM((4, 2, 8, 128, 128), F32),
            pltpu.VMEM((2, 8, 128, 128), F32),
            pltpu.VMEM((4, 2, 8, 64, 128), F32),
            pltpu.VMEM((2, 8, 64, 128), F32),
            pltpu.VMEM((3, 2, 8, 64, 128), F32),
            pltpu.VMEM((2, 8, 64, 128), F32),
            pltpu.VMEM((3, 2, 8, 64, 128), F32),
            pltpu.VMEM((2, 2, 4, 64, 128), F32),
            pltpu.VMEM((2, 512, 128), F32),
            pltpu.VMEM((3, 2, 512, 128), F32),
            pltpu.VMEM((2, 512, 128), F32),
            pltpu.VMEM((3, 2, 512, 128), F32),
            pltpu.VMEM((3, 128, 512), F32),
            pltpu.VMEM((2, 128, 512), F32),
            pltpu.VMEM((3, 512, 256), F32),
            pltpu.VMEM((3, 512, 256), F32),
            pltpu.VMEM((2, 5, 6, 48, 256), F32),
            pltpu.VMEM((3, 6, 6, 48, 256), F32),
            pltpu.VMEM((2, 512, 512), F32),
            pltpu.VMEM((512, 512), F32),
            pltpu.VMEM((3, 512, 512), BF16),
            pltpu.VMEM((3, 512, 512), BF16),
            dma((4, 2, 8, 6)),
            dma((4, 2, 8, 6)),
            dma((3, 2, 4, 2)),
            dma((3, 2, 4, 2)),
            dma((8, 2)),
            dma((8, 2)),
            dma,
            dma,
            dma((2, 8)),
            dma((2, 2, 4)),
            dma((3,)),
            dma((3,)),
            dma((3, 6, 7)),
            dma((3, 6, 7)),
            dma((3,)),
            dma((3,)),
        ],
        compiler_params=pltpu.CompilerParams(has_side_effects=True, collective_id=0, vmem_limit_bytes=VMEM_LIMIT),
    )(interval, matrix, slab)


def shards(matrix, start_vectors, interval):
    return chain_call(matrix, start_vectors, interval)


def solution(mesh):
    torus = Mesh(mesh.devices.reshape(4, 2, 4, 4), ("row_0", "row_1", "col_0", "col_1"))
    placed = (P(ROW, COL), P(COL_ROW, None), P())
    return jax.shard_map(
        shards,
        mesh=torus,
        in_specs=placed,
        out_specs=(P(COL_ROW, None), P(), P(COL_ROW, None)),
        check_vma=False,
    )
```

```python
import jax
import jax.numpy as jnp
from jax import lax
from jax.experimental import pallas as pl
from jax.experimental.pallas import tpu as pltpu
from jax.sharding import Mesh
from jax.sharding import PartitionSpec as P

ROW = ("row_0", "row_1")
COL = ("col_0", "col_1")
COL_ROW = ("col_0", "col_1", "row_0", "row_1")
MESH = pl.DeviceIdType.MESH
F32 = jnp.float32
BF16 = jnp.bfloat16
AXES6 = ("xa", "xb", "ya", "yb", "za", "zb"), ("xb", "xa", "yb", "ya", "zb", "za")
SUM_LINKS = tuple(order[k:] + order[:k] for k in (0, 2, 4) for order in AXES6)
SUM_HALF = 48, 48, 40, 40, 40, 40
SUM_START = 0, 96, 192, 272, 352, 432
VMEM_LIMIT = 63 * 1024 * 1024
LINKS = ("ya", "yb", "za", "zb"), ("yb", "ya", "zb", "za"), ("za", "zb", "ya", "yb"), ("zb", "za", "yb", "ya")
STREAMS = LINKS + LINKS


class Place:
    def __init__(self):
        self.x = lax.axis_index("row_0")
        self.core = lax.axis_index("row_1")
        self.z = lax.axis_index("col_0")
        self.y = lax.axis_index("col_1")
        self.at = {"x": self.x, "y": self.y, "z": self.z}

    def device(self, x=None, core=None, z=None, y=None):
        pick = lambda given, own: own if given is None else given
        return (pick(x, self.x), pick(core, self.core), pick(z, self.z), pick(y, self.y))

    def sibling(self):
        return self.device(core=1 - self.core)

    def partner(self, link):
        v = self.at[link[0]]
        w = v + 1 - 2 * (v % 2) if link[1] == "a" else 3 - v
        return self.device(**{link[0]: w})

    def bit(self, link):
        v = self.at[link[0]]
        return ((v + 1) // 2) % 2 if link[1] == "a" else v // 2


def remote(src, dst, send, recv, device):
    return pltpu.make_async_remote_copy(
        src_ref=src, dst_ref=dst, send_sem=send, recv_sem=recv, device_id=device, device_id_type=MESH
    )


def rows_at(start, size):
    return pl.ds(pl.multiple_of(start, size), size)


def chosen(index, values):
    result = values[-1]
    for i, value in list(enumerate(values))[-2::-1]:
        result = jnp.where(index == i, value, result)
    return result


def lanes_at(start, size):
    return pl.ds(pl.multiple_of(start, 128), size)


def halves(value):
    hi = value.astype(BF16)
    return hi, (value - hi.astype(F32)).astype(BF16)


def dot(left, right):
    return jnp.dot(left, right, preferred_element_type=F32)


def thirds(value):
    a = value.astype(BF16)
    rest = value - a.astype(F32)
    b = rest.astype(BF16)
    return a, b, (rest - b.astype(F32)).astype(BF16)


def small_factor(tile):
    sub = lax.broadcasted_iota(jnp.int32, (8, 128), 0)
    w = [tile[8 * i : 8 * i + 8, :] for i in range(8)]
    spread = lambda value, lane: jnp.broadcast_to(value[:, lane : lane + 1], (8, 128))
    pick = lambda value, row: jnp.broadcast_to(value[row : row + 1, :], (8, 128))
    ahead = [spread(w[0], c) for c in range(8)]
    for p in range(8):
        col = {(p, c): ahead[c] for c in range(8)}
        col.update({(i, c): spread(w[i], 8 * p + c) for i in range(p + 1, 8) for c in range(8)})
        if p < 7:
            ahead = [spread(w[p + 1], 8 * p + 8 + c) for c in range(8)]
        for c in range(8):
            inv = lax.rsqrt(pick(col[p, c], c))
            row = pick(w[p], c) * inv
            own = col[p, c] * inv
            w[p] = jnp.where(sub > c, w[p] - own * row, jnp.where(sub == c, row, w[p]))
            steps = [pick(col[p, c], d) * inv for d in range(c + 1, 8)]
            for d in range(c + 1, 8):
                col[p, d] = col[p, d] - own * steps[d - c - 1]
            for i in range(p + 1, 8):
                mult = col[i, c] * inv
                w[i] = w[i] - mult * row
                for d in range(c + 1, 8):
                    col[i, d] = col[i, d] - mult * steps[d - c - 1]
                if i == p + 1:
                    ahead = [ahead[d] - mult * pick(mult, d) for d in range(8)]
    return jnp.concatenate(w, axis=0)


def factor_block(x, k):
    here = pl.ds(pl.multiple_of(64 * k, 64), 64)
    pair = pl.ds(pl.multiple_of(128 * (k // 2), 128), 128)
    odd = k % 2
    lane = lax.broadcasted_iota(jnp.int32, (64, 128), 1)
    rowi = lax.broadcasted_iota(jnp.int32, (64, 128), 0)
    a = x[here, pair]
    a = jnp.where(odd == 1, pltpu.roll(a, 64, 1), a)
    w = small_factor(jnp.where(lane < 64, a, (lane - 64 == rowi).astype(F32)))
    linv = pltpu.roll(w, 64, 1)[:, :64]
    rows = jnp.dot(linv, x[here, :], precision=lax.Precision.HIGHEST, preferred_element_type=F32)
    x[here, :] = rows
    placed = jnp.where(odd == 1, w, pltpu.roll(w, 64, 1))
    x[here, pair] = jnp.where(lane // 64 == odd, placed, x[here, pair])
    full = x[here, :]
    wide = lax.broadcasted_iota(jnp.int32, (64, 512), 1)
    left = jnp.where(wide // 64 > k, full, 0.0)
    h, m, l = thirds(full)
    lh, lm, ll = thirds(left)
    right = jnp.concatenate([h, m, h, m, l, h], axis=0)
    lefts = jnp.concatenate([lh, lh, lm, lm, lh, ll], axis=0)
    update = lax.dot_general(lefts, right, (((0,), (0,)), ((), ())), preferred_element_type=F32)
    r = lax.broadcasted_iota(jnp.int32, (512, 512), 0)
    c = lax.broadcasted_iota(jnp.int32, (512, 512), 1)
    x[...] = jnp.where((c // 64 == k) & (r // 64 > k), 0.0, x[...]) - update


def lower_only(x):
    for i in range(4):
        strip = pl.ds(128 * i, 128)
        r = 128 * i + lax.broadcasted_iota(jnp.int32, (128, 512), 0)
        c = lax.broadcasted_iota(jnp.int32, (128, 512), 1)
        x[strip, :] = jnp.where(c <= r, x[strip, :], 0.0)


def precise(lefts, rights):
    (a, b, c), (x, y, z) = lefts, rights
    return (dot(b, y) + dot(a, z) + dot(c, x)) + (dot(a, y) + dot(b, x)) + dot(a, x)


def precise_gram(lefts, rights):
    (a, b, c), (x, y, z) = lefts, rights
    tall = jnp.concatenate([a, a, b, b, a, c], axis=0)
    other = jnp.concatenate([x, y, x, y, z, x], axis=0)
    return lax.dot_general(tall, other, (((0,), (0,)), ((), ())), preferred_element_type=F32)


def chain_kernel(
    interval, matrix, slab, basis_out, proj_out, resid_out,
    other, m_hi, m_lo, t_hi, t_lo, cols, rows, part, split_c, split_r,
    r1, h1, r2, h2, r3, h3, r4, share,
    tb, rb1, tb2, rb2, full, mapped, local, total, term, got, inverse, cross, turned, parts,
    f_send, f_recv, b_send, b_recv, g_send, g_recv, m_send, m_recv, p_send, p_recv, s_send, s_recv,
    a_send, a_recv, x_send, x_recv,
):
    me = Place()
    block = me.z * 4 + me.y

    barrier = pltpu.get_barrier_semaphore()
    near = [me.device(x=(me.x + d // 2) % 4, core=(me.core + d) % 2) for d in range(1, 8)]
    near += [me.partner(link) for link in ("ya", "yb", "za", "zb")]
    for device in near:
        pl.semaphore_signal(barrier, inc=1, device_id=device, device_id_type=MESH)
    pl.semaphore_wait(barrier, len(near))

    swap = remote(matrix, other, m_send, m_recv, me.sibling())
    swap.start()

    def slab_rows(x, core):
        return rows_at((x * 2 + core) * 64, 64)

    gathers = []
    for d in range(1, 8):
        to_x, to_core = (me.x + d // 2) % 4, (me.core + d) % 2
        for c in range(2):
            copy = remote(
                slab.at[:, lanes_at(256 * to_core + 128 * c, 128)], cols.at[0, c, slab_rows(me.x, me.core)],
                g_send.at[d, c], g_recv.at[d, c], me.device(x=to_x, core=to_core),
            )
            copy.start()
            gathers.append((d, c, copy))
    for c in range(2):
        cols[0, c, slab_rows(me.x, me.core), :] = slab[:, lanes_at(256 * me.core + 128 * c, 128)]

    center = 0.5 * (interval[0] + interval[1])
    half_width = 0.5 * (interval[1] - interval[0])

    def prepare(source, half):
        def tile(i, carry):
            base = half * 1024 + i * 256
            value = source[rows_at(i * 256, 256), :]
            row = me.x * 2048 + base + lax.broadcasted_iota(jnp.int32, (256, 512), 0)
            col = block * 512 + lax.broadcasted_iota(jnp.int32, (256, 512), 1)
            value = jnp.where(row == col, value - center, value) / half_width
            hi, lo = halves(value)
            where = rows_at(base, 256)
            m_hi[where, :] = hi
            m_lo[where, :] = lo
            hi, lo = halves(value.T)
            t_hi[:, where] = hi
            t_lo[:, where] = lo
            return carry

        lax.fori_loop(0, 4, tile, 0)

    prepare(matrix, me.core)
    swap.wait()
    prepare(other, 1 - me.core)
    for d, c, copy in gathers:
        copy.wait()

    def forward(c, f, source, target, before, last=False):
        hi, lo = halves(cols[source, c])
        split_c[c, :, :128] = hi
        split_c[c, :, 128:] = lo
        copies = {}

        def send(q, step, src, dst, link):
            copies[q, step] = remote(src, dst, f_send.at[f, c, q, step], f_recv.at[f, c, q, step], me.partner(link))
            copies[q, step].start()

        def multiply(q, carry):
            strip = rows_at(512 * q, 512)
            both = split_c[c]
            product = dot(m_hi[strip, :], both) + dot(m_lo[strip, :], both)
            part[c, strip, :] = product[:, :128] + product[:, 128:]
            for u in range(2):
                links = [STREAMS[2 * i + u][0] for i in range(4)]
                k1 = chosen(q, [me.bit(link) for link in links])
                there = [chosen(q, [me.partner(link)[i] for link in links]) for i in range(4)]
                remote(
                    part.at[c, rows_at(512 * q + 256 * u + 128 * (1 - k1), 128)], r1.at[f, c, 2 * q + u],
                    f_send.at[f, c, 2 * q + u, 0], f_recv.at[f, c, 2 * q + u, 0], tuple(there),
                ).start()
            return carry

        lax.fori_loop(0, 4, multiply, 0)
        where1, where2 = [], []
        for q, (l1, l2, l3, l4) in enumerate(STREAMS):
            k1, k2 = me.bit(l1), me.bit(l2)
            where1.append(256 * q + 128 * k1)
            where2.append(256 * q + 128 * k1 + 64 * k2)
            copies[q, 0] = remote(
                part.at[c, rows_at(256 * q + 128 * (1 - k1), 128)], r1.at[f, c, q],
                f_send.at[f, c, q, 0], f_recv.at[f, c, q, 0], me.partner(l1),
            )
        yield
        for q, (l1, l2, l3, l4) in enumerate(STREAMS):
            k2 = me.bit(l2)
            copies[q, 0].wait_recv()
            h1[c, q] = part[c, rows_at(where1[q], 128), :] + r1[f, c, q]
            send(q, 1, h1.at[c, q, rows_at(64 * (1 - k2), 64)], r2.at[f, c, q], l2)
        yield
        for q, (l1, l2, l3, l4) in enumerate(STREAMS):
            k2 = me.bit(l2)
            copies[q, 1].wait_recv()
            h2[c, q] = h1[c, q, rows_at(64 * k2, 64), :] + r2[f, c, q]
            if not last:
                send(q, 2, h2.at[c, q], r3.at[f, c, q], l3)
        if last:
            for copy in copies.values():
                copy.wait_send()
            return
        yield
        for q, (l1, l2, l3, l4) in enumerate(STREAMS):
            copies[q, 2].wait_recv()
            h3[c, q] = h2[c, q] + r3[f, c, q]
            send(q, 3, h3.at[c, q], r4.at[f, c, q], l4)
        yield
        for q, (l1, l2, l3, l4) in enumerate(STREAMS):
            copies[q, 3].wait_recv()
            total = h3[c, q] + r4[f, c, q]
            here = rows_at(where2[q], 64)
            if before is not None:
                total = 2.0 * total - rows[before, c, here, :]
            rows[target, c, here, :] = total
            send(q, 4, rows.at[target, c, here], rows.at[target, c, here], l2)
        yield
        for q, (l1, l2, l3, l4) in enumerate(STREAMS):
            copies[q, 4].wait_recv()
            here = rows_at(where1[q], 128)
            send(q, 5, rows.at[target, c, here], rows.at[target, c, here], l1)
        yield
        for q in range(8):
            copies[q, 5].wait_recv()
        for copy in copies.values():
            copy.wait_send()

    def backward(c, b, source, target, before):
        def split(i, carry):
            strip = rows_at(512 * i, 512)
            hi, lo = halves(rows[source, c, strip, :])
            split_r[c, strip, :128] = hi
            split_r[c, strip, 128:] = lo
            return carry

        lax.fori_loop(0, 4, split, 0)
        orders = ("xa", "xb"), ("xb", "xa")
        copies = {}

        def send(s, step, src, dst, link):
            copies[s, step] = remote(src, dst, b_send.at[b, c, s, step], b_recv.at[b, c, s, step], me.partner(link))
            copies[s, step].start()

        def multiply(s, carry):
            strip = rows_at(256 * s, 256)
            both = split_r[c]
            product = dot(t_hi[strip, :], both) + dot(t_lo[strip, :], both)
            tb[c, strip, :] = product[:, :128] + product[:, 128:]
            for u in range(2):
                strip = rows_at(256 * s + 128 * u, 128)
                remote(
                    tb.at[c, strip], rb1.at[b, c, strip],
                    b_send.at[b, c, 2 * s + u, 0], b_recv.at[b, c, 2 * s + u, 0], me.partner(orders[u][0]),
                ).start()
            return carry

        lax.fori_loop(0, 2, multiply, 0)
        for s in range(4):
            strip = pl.ds(128 * s, 128)
            copies[s, 0] = remote(
                tb.at[c, strip], rb1.at[b, c, strip],
                b_send.at[b, c, s, 0], b_recv.at[b, c, s, 0], me.partner(orders[s % 2][0]),
            )
        yield
        for s in range(4):
            strip = pl.ds(128 * s, 128)
            copies[s, 0].wait_recv()
            tb2[c, strip, :] = tb[c, strip, :] + rb1[b, c, strip, :]
            send(s, 1, tb2.at[c, strip], rb2.at[b, c, strip], orders[s % 2][1])
        yield
        for s in range(4):
            strip = pl.ds(128 * s, 128)
            copies[s, 1].wait_recv()
            total = tb2[c, strip, :] + rb2[b, c, strip, :]
            if before is not None:
                total = 2.0 * total - cols[before, c, strip, :]
            cols[target, c, strip, :] = total
        for copy in copies.values():
            copy.wait_send()

    done = set()

    def chain(c):
        yield from forward(c, 0, 0, 0, None)
        yield from backward(c, 0, 0, 1, 0)
        yield from forward(c, 1, 1, 1, 0)
        done.add(("y3", c))
        yield from backward(c, 1, 1, 2, None)
        yield from forward(c, 2, 2, 2, 1)
        yield from backward(c, 2, 2, 3, 2)
        done.add(("v3", c))
        yield from forward(c, 3, 3, None, None, last=True)
        mine = lanes_at(256 * me.core + 128 * c, 128)
        pending = []
        own_index = None
        for q, (l1, l2, l3, l4) in enumerate(STREAMS):
            k1, k2, k3, k4 = me.bit(l1), me.bit(l2), me.bit(l3), me.bit(l4)
            to_x, to_y, to_z = 2 * (q % 2) + k1, q // 2, me.x
            index = 2 * k3 + k4
            same = (to_x == me.x) & (to_y == me.y) & (to_z == me.z)
            own_index = jnp.where(same, 4 * k2 + index, -1 if own_index is None else own_index)
            copy = remote(
                h2.at[c, q], share.at[c, k2, index],
                p_send.at[c, q], p_recv.at[c, k2, index], me.device(x=to_x, y=to_y, z=to_z),
            )

            @pl.when(jnp.logical_not(same))
            def _():
                copy.start()

            @pl.when(same)
            def _():
                share[c, k2, index] = h2[c, q]

            pending.append((same, copy))
        yield
        for same, copy in pending:

            @pl.when(jnp.logical_not(same))
            def _():
                copy.wait_send()

        for k2 in range(2):
            for index in range(4):

                @pl.when(own_index != 4 * k2 + index)
                def _():
                    remote(
                        h2.at[c, 0], share.at[c, k2, index], p_send.at[c, 0], p_recv.at[c, k2, index], me.sibling()
                    ).wait_recv()

            pieces = [share[c, k2, index] for index in range(4)]
            full[2, pl.ds(64 * k2, 64), mine] = (pieces[0] + pieces[1]) + (pieces[2] + pieces[3])
        done.add(("z2", c))

    half = lanes_at(256 * me.core, 256)

    def needs(*marks):
        while not all(mark in done for mark in marks):
            yield "blocked"

    def swap_slab(k):
        copy = remote(full.at[k, :, half], full.at[k, :, half], s_send.at[k], s_recv.at[k], me.sibling())
        copy.start()
        yield
        copy.wait()

    def all_sum(n, target):
        def piece(s, k):
            return pl.ds(pl.multiple_of(SUM_START[s] + SUM_HALF[s] * k, 8), SUM_HALF[s])

        small = [pl.ds(0, SUM_HALF[s]) for s in range(6)]
        keep = [piece(s, me.bit(order[0])) for s, order in enumerate(SUM_LINKS)]
        away = [piece(s, 1 - me.bit(order[0])) for s, order in enumerate(SUM_LINKS)]
        copies = {}
        for s, order in enumerate(SUM_LINKS):
            for t in range(7):
                if t == 0:
                    src, dst = local.at[n, away[s]], got.at[n, 0, s, small[s]]
                elif t < 6:
                    src, dst = term.at[n % 2, t - 1, s, small[s]], got.at[n, t, s, small[s]]
                else:
                    src = dst = total.at[n, keep[s]]
                link = order[t % 6]
                copies[s, t] = remote(src, dst, a_send.at[n, s, t], a_recv.at[n, s, t], me.partner(link))
        copy = remote(total.at[n], target.at[:, half], x_send.at[n], x_recv.at[n], me.sibling())
        for s in range(6):
            copies[s, 0].start()
        yield
        for t in range(1, 6):
            for s in range(6):
                copies[s, t - 1].wait_recv()
                before = local[n, keep[s], :] if t == 1 else term[n % 2, t - 2, s, small[s], :]
                term[n % 2, t - 1, s, small[s], :] = before + got[n, t - 1, s, small[s], :]
                copies[s, t].start()
            yield
        for s in range(6):
            copies[s, 5].wait_recv()
            total[n, keep[s], :] = term[n % 2, 4, s, small[s], :] + got[n, 5, s, small[s], :]
            copies[s, 6].start()
        yield
        for s in range(6):
            copies[s, 6].wait_recv()
        copy.start()
        target[:, half] = total[n]
        for one in copies.values():
            one.wait_send()
        yield
        copy.wait()

    def keep_transposed(x):
        for i, one in enumerate(thirds(x[...].T)):
            turned[i] = one

    def transposed():
        return turned[0], turned[1], turned[2]

    def first_factor():
        yield from needs(("y3", 0), ("y3", 1))
        for c in range(2):
            full[0, :, lanes_at(256 * me.core + 128 * c, 128)] = rows[1, c, rows_at(block * 128, 128), :]
        yield from swap_slab(0)
        local[0] = precise_gram(thirds(full[0]), thirds(full[0, :, half])) / 8192
        yield from all_sum(0, inverse.at[0])
        for k in range(8):
            factor_block(inverse.at[0], jnp.int32(k))
            yield
        lower_only(inverse.at[0])
        keep_transposed(inverse.at[0])
        done.add("first")

    def second_factor():
        yield from needs(("v3", 0), ("v3", 1))
        for c in range(2):
            full[1, :, lanes_at(256 * me.core + 128 * c, 128)] = cols[3, c, rows_at(me.x * 128, 128), :]
        yield from swap_slab(1)
        yield from needs("first")
        mapped[0] = precise(thirds(full[1]), transposed())
        local[1] = precise_gram(thirds(mapped[0]), thirds(mapped[0, :, half])) / 8192
        done.add("filtered")
        yield from all_sum(1, inverse.at[1])

    def cross_terms():
        yield from needs(("z2", 0), ("z2", 1), "filtered")
        yield from swap_slab(2)
        mapped[1] = precise(thirds(full[2]), transposed())
        local[2] = precise_gram(thirds(mapped[0]), thirds(mapped[1, :, half])) / 8192
        yield from all_sum(2, cross)

    crossing = cross_terms()
    live = [chain(0), chain(1), first_factor(), second_factor(), crossing]
    while len(live) > 1:
        for one in list(live):
            if next(one, "end") == "end":
                live.remove(one)

    def factor_and_cross(k, carry):
        factor_block(inverse.at[1], k)
        for i in range(8):

            @pl.when(k == i)
            def _():
                next(crossing, "end")

        return carry

    lax.fori_loop(0, 8, factor_and_cross, 0)
    for _ in crossing:
        pass
    lower_only(inverse.at[1])

    keep_transposed(inverse.at[1])
    mine = rows_at(64 * me.core, 64)
    basis = precise(thirds(mapped[0, mine, :]), transposed())
    basis_out[...] = basis
    for i, one in enumerate(thirds(cross[...])):
        parts[i] = one

    def solve_left(i, carry):
        strip = rows_at(256 * i, 256)
        cross[strip, :] = precise(thirds(inverse[1, strip, :]), (parts[0], parts[1], parts[2]))
        return carry

    lax.fori_loop(0, 2, solve_left, 0)

    def solve_right(i, carry):
        strip = rows_at(256 * i, 256)
        proj_out[strip, :] = precise(thirds(cross[strip, :]), transposed())
        return carry

    lax.fori_loop(0, 2, solve_right, 0)
    rest = mapped[1, mine, :] - precise(thirds(basis), thirds(cross[...]))
    resid_out[...] = precise(thirds(rest), transposed())


def chain_call(matrix, slab, interval):
    vm = pl.BlockSpec(memory_space=pltpu.VMEM)
    dma = pltpu.SemaphoreType.DMA
    slab_shape = jax.ShapeDtypeStruct((64, 512), F32)
    return pl.pallas_call(
        chain_kernel,
        out_shape=(slab_shape, jax.ShapeDtypeStruct((512, 512), F32), slab_shape),
        in_specs=[pl.BlockSpec(memory_space=pltpu.SMEM), vm, vm],
        out_specs=(vm, vm, vm),
        scratch_shapes=[
            pltpu.VMEM((1024, 512), F32),
            pltpu.VMEM((2048, 512), BF16),
            pltpu.VMEM((2048, 512), BF16),
            pltpu.VMEM((512, 2048), BF16),
            pltpu.VMEM((512, 2048), BF16),
            pltpu.VMEM((4, 2, 512, 128), F32),
            pltpu.VMEM((3, 2, 2048, 128), F32),
            pltpu.VMEM((2, 2048, 128), F32),
            pltpu.VMEM((2, 512, 256), BF16),
            pltpu.VMEM((2, 2048, 256), BF16),
            pltpu.VMEM((4, 2, 8, 128, 128), F32),
            pltpu.VMEM((2, 8, 128, 128), F32),
            pltpu.VMEM((4, 2, 8, 64, 128), F32),
            pltpu.VMEM((2, 8, 64, 128), F32),
            pltpu.VMEM((3, 2, 8, 64, 128), F32),
            pltpu.VMEM((2, 8, 64, 128), F32),
            pltpu.VMEM((3, 2, 8, 64, 128), F32),
            pltpu.VMEM((2, 2, 4, 64, 128), F32),
            pltpu.VMEM((2, 512, 128), F32),
            pltpu.VMEM((3, 2, 512, 128), F32),
            pltpu.VMEM((2, 512, 128), F32),
            pltpu.VMEM((3, 2, 512, 128), F32),
            pltpu.VMEM((3, 128, 512), F32),
            pltpu.VMEM((2, 128, 512), F32),
            pltpu.VMEM((3, 512, 256), F32),
            pltpu.VMEM((3, 512, 256), F32),
            pltpu.VMEM((2, 5, 6, 48, 256), F32),
            pltpu.VMEM((3, 6, 6, 48, 256), F32),
            pltpu.VMEM((2, 512, 512), F32),
            pltpu.VMEM((512, 512), F32),
            pltpu.VMEM((3, 512, 512), BF16),
            pltpu.VMEM((3, 512, 512), BF16),
            dma((4, 2, 8, 6)),
            dma((4, 2, 8, 6)),
            dma((3, 2, 4, 2)),
            dma((3, 2, 4, 2)),
            dma((8, 2)),
            dma((8, 2)),
            dma,
            dma,
            dma((2, 8)),
            dma((2, 2, 4)),
            dma((3,)),
            dma((3,)),
            dma((3, 6, 7)),
            dma((3, 6, 7)),
            dma((3,)),
            dma((3,)),
        ],
        compiler_params=pltpu.CompilerParams(has_side_effects=True, collective_id=0, vmem_limit_bytes=VMEM_LIMIT),
    )(interval, matrix, slab)


def shards(matrix, start_vectors, interval):
    return chain_call(matrix, start_vectors, interval)


def solution(mesh):
    torus = Mesh(mesh.devices.reshape(4, 2, 4, 4), ("row_0", "row_1", "col_0", "col_1"))
    placed = (P(ROW, COL), P(COL_ROW, None), P())
    return jax.shard_map(
        shards,
        mesh=torus,
        in_specs=placed,
        out_specs=(P(COL_ROW, None), P(), P(COL_ROW, None)),
        check_vma=False,
    )
```

```python
import jax
import jax.numpy as jnp
from jax import lax
from jax.experimental import pallas as pl
from jax.experimental.pallas import tpu as pltpu
from jax.sharding import Mesh
from jax.sharding import PartitionSpec as P

ROW = ("row_0", "row_1")
COL = ("col_0", "col_1")
COL_ROW = ("col_0", "col_1", "row_0", "row_1")
MESH = pl.DeviceIdType.MESH
F32 = jnp.float32
BF16 = jnp.bfloat16
AXES6 = ("xa", "xb", "ya", "yb", "za", "zb"), ("xb", "xa", "yb", "ya", "zb", "za")
SUM_LINKS = tuple(order[k:] + order[:k] for k in (0, 2, 4) for order in AXES6)
SUM_HALF = 48, 48, 40, 40, 40, 40
SUM_START = 0, 96, 192, 272, 352, 432
VMEM_LIMIT = 63 * 1024 * 1024
LINKS = ("ya", "yb", "za", "zb"), ("yb", "ya", "zb", "za"), ("za", "zb", "ya", "yb"), ("zb", "za", "yb", "ya")
STREAMS = LINKS + LINKS


class Place:
    def __init__(self):
        self.x = lax.axis_index("row_0")
        self.core = lax.axis_index("row_1")
        self.z = lax.axis_index("col_0")
        self.y = lax.axis_index("col_1")
        self.at = {"x": self.x, "y": self.y, "z": self.z}

    def device(self, x=None, core=None, z=None, y=None):
        pick = lambda given, own: own if given is None else given
        return (pick(x, self.x), pick(core, self.core), pick(z, self.z), pick(y, self.y))

    def sibling(self):
        return self.device(core=1 - self.core)

    def partner(self, link):
        v = self.at[link[0]]
        w = v + 1 - 2 * (v % 2) if link[1] == "a" else 3 - v
        return self.device(**{link[0]: w})

    def bit(self, link):
        v = self.at[link[0]]
        return ((v + 1) // 2) % 2 if link[1] == "a" else v // 2


def remote(src, dst, send, recv, device):
    return pltpu.make_async_remote_copy(
        src_ref=src, dst_ref=dst, send_sem=send, recv_sem=recv, device_id=device, device_id_type=MESH
    )


def rows_at(start, size):
    return pl.ds(pl.multiple_of(start, size), size)


def chosen(index, values):
    result = values[-1]
    for i, value in list(enumerate(values))[-2::-1]:
        result = jnp.where(index == i, value, result)
    return result


def lanes_at(start, size):
    return pl.ds(pl.multiple_of(start, 128), size)


def halves(value):
    hi = value.astype(BF16)
    return hi, (value - hi.astype(F32)).astype(BF16)


def dot(left, right):
    return jnp.dot(left, right, preferred_element_type=F32)


def thirds(value):
    a = value.astype(BF16)
    rest = value - a.astype(F32)
    b = rest.astype(BF16)
    return a, b, (rest - b.astype(F32)).astype(BF16)


def small_factor(tile):
    sub = lax.broadcasted_iota(jnp.int32, (8, 128), 0)
    w = [tile[8 * i : 8 * i + 8, :] for i in range(8)]
    spread = lambda value, lane: jnp.broadcast_to(value[:, lane : lane + 1], (8, 128))
    pick = lambda value, row: jnp.broadcast_to(value[row : row + 1, :], (8, 128))
    ahead = [spread(w[0], c) for c in range(8)]
    for p in range(8):
        col = {(p, c): ahead[c] for c in range(8)}
        col.update({(i, c): spread(w[i], 8 * p + c) for i in range(p + 1, 8) for c in range(8)})
        if p < 7:
            ahead = [spread(w[p + 1], 8 * p + 8 + c) for c in range(8)]
        for c in range(8):
            inv = lax.rsqrt(pick(col[p, c], c))
            row = pick(w[p], c) * inv
            own = col[p, c] * inv
            w[p] = jnp.where(sub > c, w[p] - own * row, jnp.where(sub == c, row, w[p]))
            steps = [pick(col[p, c], d) * inv for d in range(c + 1, 8)]
            for d in range(c + 1, 8):
                col[p, d] = col[p, d] - own * steps[d - c - 1]
            for i in range(p + 1, 8):
                mult = col[i, c] * inv
                w[i] = w[i] - mult * row
                for d in range(c + 1, 8):
                    col[i, d] = col[i, d] - mult * steps[d - c - 1]
                if i == p + 1:
                    ahead = [ahead[d] - mult * pick(mult, d) for d in range(8)]
    return jnp.concatenate(w, axis=0)


def factor_block(x, k, below=0):
    here = pl.ds(pl.multiple_of(64 * k, 64), 64)
    pair = pl.ds(pl.multiple_of(128 * (k // 2), 128), 128)
    odd = k % 2
    lane = lax.broadcasted_iota(jnp.int32, (64, 128), 1)
    rowi = lax.broadcasted_iota(jnp.int32, (64, 128), 0)
    a = x[here, pair]
    a = jnp.where(odd == 1, pltpu.roll(a, 64, 1), a)
    w = small_factor(jnp.where(lane < 64, a, (lane - 64 == rowi).astype(F32)))
    linv = pltpu.roll(w, 64, 1)[:, :64]
    rows = jnp.dot(linv, x[here, :], precision=lax.Precision.HIGHEST, preferred_element_type=F32)
    x[here, :] = rows
    placed = jnp.where(odd == 1, w, pltpu.roll(w, 64, 1))
    x[here, pair] = jnp.where(lane // 64 == odd, placed, x[here, pair])
    full = x[here, :]
    wide = lax.broadcasted_iota(jnp.int32, (64, 512), 1)
    left = jnp.where(wide // 64 > k, full, 0.0)
    h, m, l = thirds(full)
    lh, lm, ll = thirds(left)
    right = jnp.concatenate([h, m, h, m, l, h], axis=0)
    lefts = jnp.concatenate([lh, lh, lm, lm, lh, ll], axis=0)
    if below == 512:
        return
    update = lax.dot_general(lefts[:, below:], right, (((0,), (0,)), ((), ())), preferred_element_type=F32)
    r = below + lax.broadcasted_iota(jnp.int32, (512 - below, 512), 0)
    c = lax.broadcasted_iota(jnp.int32, (512 - below, 512), 1)
    x[below:, :] = jnp.where((c // 64 == k) & (r // 64 > k), 0.0, x[below:, :]) - update


def lower_only(x):
    for i in range(4):
        strip = pl.ds(128 * i, 128)
        r = 128 * i + lax.broadcasted_iota(jnp.int32, (128, 512), 0)
        c = lax.broadcasted_iota(jnp.int32, (128, 512), 1)
        x[strip, :] = jnp.where(c <= r, x[strip, :], 0.0)


def precise(lefts, rights):
    (a, b, c), (x, y, z) = lefts, rights
    return (dot(b, y) + dot(a, z) + dot(c, x)) + (dot(a, y) + dot(b, x)) + dot(a, x)


def precise_gram(lefts, rights):
    (a, b, c), (x, y, z) = lefts, rights
    tall = jnp.concatenate([a, a, b, b, a, c], axis=0)
    other = jnp.concatenate([x, y, x, y, z, x], axis=0)
    return lax.dot_general(tall, other, (((0,), (0,)), ((), ())), preferred_element_type=F32)


def chain_kernel(
    interval, matrix, slab, basis_out, proj_out, resid_out,
    other, m_hi, m_lo, t_hi, t_lo, cols, rows, part, split_c, split_r,
    r1, h1, r2, h2, r3, h3, r4, share,
    tb, rb1, tb2, rb2, full, mapped, local, total, term, got, inverse, cross, turned, parts,
    f_send, f_recv, b_send, b_recv, g_send, g_recv, m_send, m_recv, p_send, p_recv, s_send, s_recv,
    a_send, a_recv, x_send, x_recv,
):
    me = Place()
    block = me.z * 4 + me.y

    barrier = pltpu.get_barrier_semaphore()
    near = [me.device(x=(me.x + d // 2) % 4, core=(me.core + d) % 2) for d in range(1, 8)]
    near += [me.partner(link) for link in ("ya", "yb", "za", "zb")]
    for device in near:
        pl.semaphore_signal(barrier, inc=1, device_id=device, device_id_type=MESH)
    pl.semaphore_wait(barrier, len(near))

    swap = remote(matrix, other, m_send, m_recv, me.sibling())
    swap.start()

    def slab_rows(x, core):
        return rows_at((x * 2 + core) * 64, 64)

    gathers = []
    for d in range(1, 8):
        to_x, to_core = (me.x + d // 2) % 4, (me.core + d) % 2
        for c in range(2):
            copy = remote(
                slab.at[:, lanes_at(256 * to_core + 128 * c, 128)], cols.at[0, c, slab_rows(me.x, me.core)],
                g_send.at[d, c], g_recv.at[d, c], me.device(x=to_x, core=to_core),
            )
            copy.start()
            gathers.append((d, c, copy))
    for c in range(2):
        cols[0, c, slab_rows(me.x, me.core), :] = slab[:, lanes_at(256 * me.core + 128 * c, 128)]

    center = 0.5 * (interval[0] + interval[1])
    half_width = 0.5 * (interval[1] - interval[0])

    def prepare(source, half):
        def tile(i, carry):
            base = half * 1024 + i * 256
            value = source[rows_at(i * 256, 256), :]
            row = me.x * 2048 + base + lax.broadcasted_iota(jnp.int32, (256, 512), 0)
            col = block * 512 + lax.broadcasted_iota(jnp.int32, (256, 512), 1)
            value = jnp.where(row == col, value - center, value) / half_width
            hi, lo = halves(value)
            where = rows_at(base, 256)
            m_hi[where, :] = hi
            m_lo[where, :] = lo
            hi, lo = halves(value.T)
            t_hi[:, where] = hi
            t_lo[:, where] = lo
            return carry

        lax.fori_loop(0, 4, tile, 0)

    prepare(matrix, me.core)
    swap.wait()
    prepare(other, 1 - me.core)
    for d, c, copy in gathers:
        copy.wait()

    def forward(c, f, source, target, before, last=False):
        hi, lo = halves(cols[source, c])
        split_c[c, :, :128] = hi
        split_c[c, :, 128:] = lo
        copies = {}

        def send(q, step, src, dst, link):
            copies[q, step] = remote(src, dst, f_send.at[f, c, q, step], f_recv.at[f, c, q, step], me.partner(link))
            copies[q, step].start()

        def multiply(q, carry):
            strip = rows_at(512 * q, 512)
            both = split_c[c]
            product = dot(m_hi[strip, :], both) + dot(m_lo[strip, :], both)
            part[c, strip, :] = product[:, :128] + product[:, 128:]
            for u in range(2):
                links = [STREAMS[2 * i + u][0] for i in range(4)]
                k1 = chosen(q, [me.bit(link) for link in links])
                there = [chosen(q, [me.partner(link)[i] for link in links]) for i in range(4)]
                remote(
                    part.at[c, rows_at(512 * q + 256 * u + 128 * (1 - k1), 128)], r1.at[f, c, 2 * q + u],
                    f_send.at[f, c, 2 * q + u, 0], f_recv.at[f, c, 2 * q + u, 0], tuple(there),
                ).start()
            return carry

        lax.fori_loop(0, 4, multiply, 0)
        where1, where2 = [], []
        for q, (l1, l2, l3, l4) in enumerate(STREAMS):
            k1, k2 = me.bit(l1), me.bit(l2)
            where1.append(256 * q + 128 * k1)
            where2.append(256 * q + 128 * k1 + 64 * k2)
            copies[q, 0] = remote(
                part.at[c, rows_at(256 * q + 128 * (1 - k1), 128)], r1.at[f, c, q],
                f_send.at[f, c, q, 0], f_recv.at[f, c, q, 0], me.partner(l1),
            )
        yield
        for q, (l1, l2, l3, l4) in enumerate(STREAMS):
            k2 = me.bit(l2)
            copies[q, 0].wait_recv()
            h1[c, q] = part[c, rows_at(where1[q], 128), :] + r1[f, c, q]
            send(q, 1, h1.at[c, q, rows_at(64 * (1 - k2), 64)], r2.at[f, c, q], l2)
        yield
        for q, (l1, l2, l3, l4) in enumerate(STREAMS):
            k2 = me.bit(l2)
            copies[q, 1].wait_recv()
            h2[c, q] = h1[c, q, rows_at(64 * k2, 64), :] + r2[f, c, q]
            if not last:
                send(q, 2, h2.at[c, q], r3.at[f, c, q], l3)
        if last:
            for copy in copies.values():
                copy.wait_send()
            return
        yield
        for q, (l1, l2, l3, l4) in enumerate(STREAMS):
            copies[q, 2].wait_recv()
            h3[c, q] = h2[c, q] + r3[f, c, q]
            send(q, 3, h3.at[c, q], r4.at[f, c, q], l4)
        yield
        for q, (l1, l2, l3, l4) in enumerate(STREAMS):
            copies[q, 3].wait_recv()
            total = h3[c, q] + r4[f, c, q]
            here = rows_at(where2[q], 64)
            if before is not None:
                total = 2.0 * total - rows[before, c, here, :]
            rows[target, c, here, :] = total
            send(q, 4, rows.at[target, c, here], rows.at[target, c, here], l2)
        yield
        for q, (l1, l2, l3, l4) in enumerate(STREAMS):
            copies[q, 4].wait_recv()
            here = rows_at(where1[q], 128)
            send(q, 5, rows.at[target, c, here], rows.at[target, c, here], l1)
        yield
        for q in range(8):
            copies[q, 5].wait_recv()
        for copy in copies.values():
            copy.wait_send()

    def backward(c, b, source, target, before):
        def split(i, carry):
            strip = rows_at(512 * i, 512)
            hi, lo = halves(rows[source, c, strip, :])
            split_r[c, strip, :128] = hi
            split_r[c, strip, 128:] = lo
            return carry

        lax.fori_loop(0, 4, split, 0)
        orders = ("xa", "xb"), ("xb", "xa")
        copies = {}

        def send(s, step, src, dst, link):
            copies[s, step] = remote(src, dst, b_send.at[b, c, s, step], b_recv.at[b, c, s, step], me.partner(link))
            copies[s, step].start()

        def multiply(s, carry):
            strip = rows_at(256 * s, 256)
            both = split_r[c]
            product = dot(t_hi[strip, :], both) + dot(t_lo[strip, :], both)
            tb[c, strip, :] = product[:, :128] + product[:, 128:]
            for u in range(2):
                strip = rows_at(256 * s + 128 * u, 128)
                remote(
                    tb.at[c, strip], rb1.at[b, c, strip],
                    b_send.at[b, c, 2 * s + u, 0], b_recv.at[b, c, 2 * s + u, 0], me.partner(orders[u][0]),
                ).start()
            return carry

        lax.fori_loop(0, 2, multiply, 0)
        for s in range(4):
            strip = pl.ds(128 * s, 128)
            copies[s, 0] = remote(
                tb.at[c, strip], rb1.at[b, c, strip],
                b_send.at[b, c, s, 0], b_recv.at[b, c, s, 0], me.partner(orders[s % 2][0]),
            )
        yield
        for s in range(4):
            strip = pl.ds(128 * s, 128)
            copies[s, 0].wait_recv()
            tb2[c, strip, :] = tb[c, strip, :] + rb1[b, c, strip, :]
            send(s, 1, tb2.at[c, strip], rb2.at[b, c, strip], orders[s % 2][1])
        yield
        for s in range(4):
            strip = pl.ds(128 * s, 128)
            copies[s, 1].wait_recv()
            total = tb2[c, strip, :] + rb2[b, c, strip, :]
            if before is not None:
                total = 2.0 * total - cols[before, c, strip, :]
            cols[target, c, strip, :] = total
        for copy in copies.values():
            copy.wait_send()

    done = set()

    def chain(c):
        yield from forward(c, 0, 0, 0, None)
        yield from backward(c, 0, 0, 1, 0)
        yield from forward(c, 1, 1, 1, 0)
        done.add(("y3", c))
        yield from backward(c, 1, 1, 2, None)
        yield from forward(c, 2, 2, 2, 1)
        yield from backward(c, 2, 2, 3, 2)
        done.add(("v3", c))
        yield from forward(c, 3, 3, None, None, last=True)
        mine = lanes_at(256 * me.core + 128 * c, 128)
        pending = []
        own_index = None
        for q, (l1, l2, l3, l4) in enumerate(STREAMS):
            k1, k2, k3, k4 = me.bit(l1), me.bit(l2), me.bit(l3), me.bit(l4)
            to_x, to_y, to_z = 2 * (q % 2) + k1, q // 2, me.x
            index = 2 * k3 + k4
            same = (to_x == me.x) & (to_y == me.y) & (to_z == me.z)
            own_index = jnp.where(same, 4 * k2 + index, -1 if own_index is None else own_index)
            copy = remote(
                h2.at[c, q], share.at[c, k2, index],
                p_send.at[c, q], p_recv.at[c, k2, index], me.device(x=to_x, y=to_y, z=to_z),
            )

            @pl.when(jnp.logical_not(same))
            def _():
                copy.start()

            @pl.when(same)
            def _():
                share[c, k2, index] = h2[c, q]

            pending.append((same, copy))
        yield
        for same, copy in pending:

            @pl.when(jnp.logical_not(same))
            def _():
                copy.wait_send()

        for k2 in range(2):
            for index in range(4):

                @pl.when(own_index != 4 * k2 + index)
                def _():
                    remote(
                        h2.at[c, 0], share.at[c, k2, index], p_send.at[c, 0], p_recv.at[c, k2, index], me.sibling()
                    ).wait_recv()

            pieces = [share[c, k2, index] for index in range(4)]
            full[2, pl.ds(64 * k2, 64), mine] = (pieces[0] + pieces[1]) + (pieces[2] + pieces[3])
        done.add(("z2", c))

    half = lanes_at(256 * me.core, 256)

    def needs(*marks):
        while not all(mark in done for mark in marks):
            yield "blocked"

    def swap_slab(k):
        copy = remote(full.at[k, :, half], full.at[k, :, half], s_send.at[k], s_recv.at[k], me.sibling())
        copy.start()
        yield
        copy.wait()

    def all_sum(n, target):
        def piece(s, k):
            return pl.ds(pl.multiple_of(SUM_START[s] + SUM_HALF[s] * k, 8), SUM_HALF[s])

        small = [pl.ds(0, SUM_HALF[s]) for s in range(6)]
        keep = [piece(s, me.bit(order[0])) for s, order in enumerate(SUM_LINKS)]
        away = [piece(s, 1 - me.bit(order[0])) for s, order in enumerate(SUM_LINKS)]
        copies = {}
        for s, order in enumerate(SUM_LINKS):
            for t in range(7):
                if t == 0:
                    src, dst = local.at[n, away[s]], got.at[n, 0, s, small[s]]
                elif t < 6:
                    src, dst = term.at[n % 2, t - 1, s, small[s]], got.at[n, t, s, small[s]]
                else:
                    src = dst = total.at[n, keep[s]]
                link = order[t % 6]
                copies[s, t] = remote(src, dst, a_send.at[n, s, t], a_recv.at[n, s, t], me.partner(link))
        copy = remote(total.at[n], target.at[:, half], x_send.at[n], x_recv.at[n], me.sibling())
        for s in range(6):
            copies[s, 0].start()
        yield
        for t in range(1, 6):
            for s in range(6):
                copies[s, t - 1].wait_recv()
                before = local[n, keep[s], :] if t == 1 else term[n % 2, t - 2, s, small[s], :]
                term[n % 2, t - 1, s, small[s], :] = before + got[n, t - 1, s, small[s], :]
                copies[s, t].start()
            yield
        for s in range(6):
            copies[s, 5].wait_recv()
            total[n, keep[s], :] = term[n % 2, 4, s, small[s], :] + got[n, 5, s, small[s], :]
            copies[s, 6].start()
        yield
        for s in range(6):
            copies[s, 6].wait_recv()
        copy.start()
        target[:, half] = total[n]
        for one in copies.values():
            one.wait_send()
        yield
        copy.wait()

    def keep_transposed(x):
        for i, one in enumerate(thirds(x[...].T)):
            turned[i] = one

    def transposed():
        return turned[0], turned[1], turned[2]

    def first_factor():
        yield from needs(("y3", 0), ("y3", 1))
        for c in range(2):
            full[0, :, lanes_at(256 * me.core + 128 * c, 128)] = rows[1, c, rows_at(block * 128, 128), :]
        yield from swap_slab(0)
        local[0] = precise_gram(thirds(full[0]), thirds(full[0, :, half])) / 8192
        yield from all_sum(0, inverse.at[0])
        for k in range(8):
            factor_block(inverse.at[0], jnp.int32(k), 128 * ((k + 1) // 2))
            yield
        lower_only(inverse.at[0])
        keep_transposed(inverse.at[0])
        done.add("first")

    def second_factor():
        yield from needs(("v3", 0), ("v3", 1))
        for c in range(2):
            full[1, :, lanes_at(256 * me.core + 128 * c, 128)] = cols[3, c, rows_at(me.x * 128, 128), :]
        yield from swap_slab(1)
        yield from needs("first")
        mapped[0] = precise(thirds(full[1]), transposed())
        local[1] = precise_gram(thirds(mapped[0]), thirds(mapped[0, :, half])) / 8192
        done.add("filtered")
        yield from all_sum(1, inverse.at[1])

    def cross_terms():
        yield from needs(("z2", 0), ("z2", 1), "filtered")
        yield from swap_slab(2)
        mapped[1] = precise(thirds(full[2]), transposed())
        local[2] = precise_gram(thirds(mapped[0]), thirds(mapped[1, :, half])) / 8192
        yield from all_sum(2, cross)

    crossing = cross_terms()
    live = [chain(0), chain(1), first_factor(), second_factor(), crossing]
    while len(live) > 1:
        for one in list(live):
            if next(one, "end") == "end":
                live.remove(one)

    def factor_and_cross(k, carry):
        factor_block(inverse.at[1], k)
        for i in range(8):

            @pl.when(k == i)
            def _():
                next(crossing, "end")

        return carry

    lax.fori_loop(0, 8, factor_and_cross, 0)
    for _ in crossing:
        pass
    lower_only(inverse.at[1])

    keep_transposed(inverse.at[1])
    mine = rows_at(64 * me.core, 64)
    basis = precise(thirds(mapped[0, mine, :]), transposed())
    basis_out[...] = basis
    for i, one in enumerate(thirds(cross[...])):
        parts[i] = one

    def solve_left(i, carry):
        strip = rows_at(256 * i, 256)
        cross[strip, :] = precise(thirds(inverse[1, strip, :]), (parts[0], parts[1], parts[2]))
        return carry

    lax.fori_loop(0, 2, solve_left, 0)

    def solve_right(i, carry):
        strip = rows_at(256 * i, 256)
        proj_out[strip, :] = precise(thirds(cross[strip, :]), transposed())
        return carry

    lax.fori_loop(0, 2, solve_right, 0)
    rest = mapped[1, mine, :] - precise(thirds(basis), thirds(cross[...]))
    resid_out[...] = precise(thirds(rest), transposed())


def chain_call(matrix, slab, interval):
    vm = pl.BlockSpec(memory_space=pltpu.VMEM)
    dma = pltpu.SemaphoreType.DMA
    slab_shape = jax.ShapeDtypeStruct((64, 512), F32)
    return pl.pallas_call(
        chain_kernel,
        out_shape=(slab_shape, jax.ShapeDtypeStruct((512, 512), F32), slab_shape),
        in_specs=[pl.BlockSpec(memory_space=pltpu.SMEM), vm, vm],
        out_specs=(vm, vm, vm),
        scratch_shapes=[
            pltpu.VMEM((1024, 512), F32),
            pltpu.VMEM((2048, 512), BF16),
            pltpu.VMEM((2048, 512), BF16),
            pltpu.VMEM((512, 2048), BF16),
            pltpu.VMEM((512, 2048), BF16),
            pltpu.VMEM((4, 2, 512, 128), F32),
            pltpu.VMEM((3, 2, 2048, 128), F32),
            pltpu.VMEM((2, 2048, 128), F32),
            pltpu.VMEM((2, 512, 256), BF16),
            pltpu.VMEM((2, 2048, 256), BF16),
            pltpu.VMEM((4, 2, 8, 128, 128), F32),
            pltpu.VMEM((2, 8, 128, 128), F32),
            pltpu.VMEM((4, 2, 8, 64, 128), F32),
            pltpu.VMEM((2, 8, 64, 128), F32),
            pltpu.VMEM((3, 2, 8, 64, 128), F32),
            pltpu.VMEM((2, 8, 64, 128), F32),
            pltpu.VMEM((3, 2, 8, 64, 128), F32),
            pltpu.VMEM((2, 2, 4, 64, 128), F32),
            pltpu.VMEM((2, 512, 128), F32),
            pltpu.VMEM((3, 2, 512, 128), F32),
            pltpu.VMEM((2, 512, 128), F32),
            pltpu.VMEM((3, 2, 512, 128), F32),
            pltpu.VMEM((3, 128, 512), F32),
            pltpu.VMEM((2, 128, 512), F32),
            pltpu.VMEM((3, 512, 256), F32),
            pltpu.VMEM((3, 512, 256), F32),
            pltpu.VMEM((2, 5, 6, 48, 256), F32),
            pltpu.VMEM((3, 6, 6, 48, 256), F32),
            pltpu.VMEM((2, 512, 512), F32),
            pltpu.VMEM((512, 512), F32),
            pltpu.VMEM((3, 512, 512), BF16),
            pltpu.VMEM((3, 512, 512), BF16),
            dma((4, 2, 8, 6)),
            dma((4, 2, 8, 6)),
            dma((3, 2, 4, 2)),
            dma((3, 2, 4, 2)),
            dma((8, 2)),
            dma((8, 2)),
            dma,
            dma,
            dma((2, 8)),
            dma((2, 2, 4)),
            dma((3,)),
            dma((3,)),
            dma((3, 6, 7)),
            dma((3, 6, 7)),
            dma((3,)),
            dma((3,)),
        ],
        compiler_params=pltpu.CompilerParams(has_side_effects=True, collective_id=0, vmem_limit_bytes=VMEM_LIMIT),
    )(interval, matrix, slab)


def shards(matrix, start_vectors, interval):
    return chain_call(matrix, start_vectors, interval)


def solution(mesh):
    torus = Mesh(mesh.devices.reshape(4, 2, 4, 4), ("row_0", "row_1", "col_0", "col_1"))
    placed = (P(ROW, COL), P(COL_ROW, None), P())
    return jax.shard_map(
        shards,
        mesh=torus,
        in_specs=placed,
        out_specs=(P(COL_ROW, None), P(), P(COL_ROW, None)),
        check_vma=False,
    )
```

```python
import jax
import jax.numpy as jnp
from jax import lax
from jax.experimental import pallas as pl
from jax.experimental.pallas import tpu as pltpu
from jax.sharding import Mesh
from jax.sharding import PartitionSpec as P

ROW = ("row_0", "row_1")
COL = ("col_0", "col_1")
COL_ROW = ("col_0", "col_1", "row_0", "row_1")
MESH = pl.DeviceIdType.MESH
F32 = jnp.float32
BF16 = jnp.bfloat16
AXES6 = ("xa", "xb", "ya", "yb", "za", "zb"), ("xb", "xa", "yb", "ya", "zb", "za")
SUM_LINKS = tuple(order[k:] + order[:k] for k in (0, 2, 4) for order in AXES6)
SUM_HALF = 48, 48, 40, 40, 40, 40
SUM_START = 0, 96, 192, 272, 352, 432
VMEM_LIMIT = 63 * 1024 * 1024
LINKS = ("ya", "yb", "za", "zb"), ("yb", "ya", "zb", "za"), ("za", "zb", "ya", "yb"), ("zb", "za", "yb", "ya")
STREAMS = LINKS + LINKS


class Place:
    def __init__(self):
        self.x = lax.axis_index("row_0")
        self.core = lax.axis_index("row_1")
        self.z = lax.axis_index("col_0")
        self.y = lax.axis_index("col_1")
        self.at = {"x": self.x, "y": self.y, "z": self.z}

    def device(self, x=None, core=None, z=None, y=None):
        pick = lambda given, own: own if given is None else given
        return (pick(x, self.x), pick(core, self.core), pick(z, self.z), pick(y, self.y))

    def sibling(self):
        return self.device(core=1 - self.core)

    def partner(self, link):
        v = self.at[link[0]]
        w = v + 1 - 2 * (v % 2) if link[1] == "a" else 3 - v
        return self.device(**{link[0]: w})

    def bit(self, link):
        v = self.at[link[0]]
        return ((v + 1) // 2) % 2 if link[1] == "a" else v // 2


def remote(src, dst, send, recv, device):
    return pltpu.make_async_remote_copy(
        src_ref=src, dst_ref=dst, send_sem=send, recv_sem=recv, device_id=device, device_id_type=MESH
    )


def rows_at(start, size):
    return pl.ds(pl.multiple_of(start, size), size)


def chosen(index, values):
    result = values[-1]
    for i, value in list(enumerate(values))[-2::-1]:
        result = jnp.where(index == i, value, result)
    return result


def lanes_at(start, size):
    return pl.ds(pl.multiple_of(start, 128), size)


def halves(value):
    hi = value.astype(BF16)
    return hi, (value - hi.astype(F32)).astype(BF16)


def dot(left, right):
    return jnp.dot(left, right, preferred_element_type=F32)


def thirds(value):
    a = value.astype(BF16)
    rest = value - a.astype(F32)
    b = rest.astype(BF16)
    return a, b, (rest - b.astype(F32)).astype(BF16)


def small_factor(tile):
    sub = lax.broadcasted_iota(jnp.int32, (8, 128), 0)
    w = [tile[8 * i : 8 * i + 8, :] for i in range(8)]
    spread = lambda value, lane: jnp.broadcast_to(value[:, lane : lane + 1], (8, 128))
    pick = lambda value, row: jnp.broadcast_to(value[row : row + 1, :], (8, 128))
    ahead = [spread(w[0], c) for c in range(8)]
    for p in range(8):
        col = {(p, c): ahead[c] for c in range(8)}
        col.update({(i, c): spread(w[i], 8 * p + c) for i in range(p + 1, 8) for c in range(8)})
        if p < 7:
            ahead = [spread(w[p + 1], 8 * p + 8 + c) for c in range(8)]
        for c in range(8):
            inv = lax.rsqrt(pick(col[p, c], c))
            row = pick(w[p], c) * inv
            own = col[p, c] * inv
            w[p] = jnp.where(sub > c, w[p] - own * row, jnp.where(sub == c, row, w[p]))
            steps = [pick(col[p, c], d) * inv for d in range(c + 1, 8)]
            for d in range(c + 1, 8):
                col[p, d] = col[p, d] - own * steps[d - c - 1]
            for i in range(p + 1, 8):
                mult = col[i, c] * inv
                w[i] = w[i] - mult * row
                for d in range(c + 1, 8):
                    col[i, d] = col[i, d] - mult * steps[d - c - 1]
                if i == p + 1:
                    ahead = [ahead[d] - mult * pick(mult, d) for d in range(8)]
    return jnp.concatenate(w, axis=0)


def factor_block(x, k, below=0):
    here = pl.ds(pl.multiple_of(64 * k, 64), 64)
    pair = pl.ds(pl.multiple_of(128 * (k // 2), 128), 128)
    odd = k % 2
    lane = lax.broadcasted_iota(jnp.int32, (64, 128), 1)
    rowi = lax.broadcasted_iota(jnp.int32, (64, 128), 0)
    a = x[here, pair]
    a = jnp.where(odd == 1, pltpu.roll(a, 64, 1), a)
    w = small_factor(jnp.where(lane < 64, a, (lane - 64 == rowi).astype(F32)))
    linv = pltpu.roll(w, 64, 1)[:, :64]
    rows = jnp.dot(linv, x[here, :], precision=lax.Precision.HIGHEST, preferred_element_type=F32)
    x[here, :] = rows
    placed = jnp.where(odd == 1, w, pltpu.roll(w, 64, 1))
    x[here, pair] = jnp.where(lane // 64 == odd, placed, x[here, pair])
    full = x[here, :]
    wide = lax.broadcasted_iota(jnp.int32, (64, 512), 1)
    left = jnp.where(wide // 64 > k, full, 0.0)
    h, m, l = thirds(full)
    lh, lm, ll = thirds(left)
    right = jnp.concatenate([h, m, h, m, l, h], axis=0)
    lefts = jnp.concatenate([lh, lh, lm, lm, lh, ll], axis=0)
    if below == 512:
        return
    update = lax.dot_general(lefts[:, below:], right, (((0,), (0,)), ((), ())), preferred_element_type=F32)
    r = below + lax.broadcasted_iota(jnp.int32, (512 - below, 512), 0)
    c = lax.broadcasted_iota(jnp.int32, (512 - below, 512), 1)
    x[below:, :] = jnp.where((c // 64 == k) & (r // 64 > k), 0.0, x[below:, :]) - update


def lower_only(x):
    for i in range(4):
        strip = pl.ds(128 * i, 128)
        r = 128 * i + lax.broadcasted_iota(jnp.int32, (128, 512), 0)
        c = lax.broadcasted_iota(jnp.int32, (128, 512), 1)
        x[strip, :] = jnp.where(c <= r, x[strip, :], 0.0)


def precise(lefts, rights):
    (a, b, c), (x, y, z) = lefts, rights
    return (dot(b, y) + dot(a, z) + dot(c, x)) + (dot(a, y) + dot(b, x)) + dot(a, x)


def precise_gram(lefts, rights):
    (a, b, c), (x, y, z) = lefts, rights
    tall = jnp.concatenate([a, a, b, b, a, c], axis=0)
    other = jnp.concatenate([x, y, x, y, z, x], axis=0)
    return lax.dot_general(tall, other, (((0,), (0,)), ((), ())), preferred_element_type=F32)


def chain_kernel(
    interval, matrix, slab, basis_out, proj_out, resid_out,
    other, m_hi, m_lo, t_hi, t_lo, cols, rows, part, split_c, split_r,
    r1, h1, r2, h2, r3, h3, r4, share,
    tb, rb1, tb2, rb2, full, mapped, local, total, term, got, inverse, cross, turned, parts,
    f_send, f_recv, b_send, b_recv, g_send, g_recv, m_send, m_recv, p_send, p_recv, s_send, s_recv,
    a_send, a_recv, x_send, x_recv,
):
    me = Place()
    block = me.z * 4 + me.y

    barrier = pltpu.get_barrier_semaphore()
    near = [me.device(x=(me.x + d // 2) % 4, core=(me.core + d) % 2) for d in range(1, 8)]
    near += [me.partner(link) for link in ("ya", "yb", "za", "zb")]
    for device in near:
        pl.semaphore_signal(barrier, inc=1, device_id=device, device_id_type=MESH)
    pl.semaphore_wait(barrier, len(near))

    swap = remote(matrix, other, m_send, m_recv, me.sibling())
    swap.start()

    def slab_rows(x, core):
        return rows_at((x * 2 + core) * 64, 64)

    gathers = []
    for d in range(1, 8):
        to_x, to_core = (me.x + d // 2) % 4, (me.core + d) % 2
        for c in range(2):
            copy = remote(
                slab.at[:, lanes_at(256 * to_core + 128 * c, 128)], cols.at[0, c, slab_rows(me.x, me.core)],
                g_send.at[d, c], g_recv.at[d, c], me.device(x=to_x, core=to_core),
            )
            copy.start()
            gathers.append((d, c, copy))
    for c in range(2):
        cols[0, c, slab_rows(me.x, me.core), :] = slab[:, lanes_at(256 * me.core + 128 * c, 128)]

    center = 0.5 * (interval[0] + interval[1])
    half_width = 0.5 * (interval[1] - interval[0])

    def prepare(source, half):
        def tile(i, carry):
            base = half * 1024 + i * 256
            value = source[rows_at(i * 256, 256), :]
            row = me.x * 2048 + base + lax.broadcasted_iota(jnp.int32, (256, 512), 0)
            col = block * 512 + lax.broadcasted_iota(jnp.int32, (256, 512), 1)
            value = jnp.where(row == col, value - center, value) / half_width
            hi, lo = halves(value)
            where = rows_at(base, 256)
            m_hi[where, :] = hi
            m_lo[where, :] = lo
            hi, lo = halves(value.T)
            t_hi[:, where] = hi
            t_lo[:, where] = lo
            return carry

        lax.fori_loop(0, 4, tile, 0)

    prepare(matrix, me.core)
    swap.wait()
    prepare(other, 1 - me.core)
    for d, c, copy in gathers:
        copy.wait()

    def forward(c, f, source, target, before, last=False):
        hi, lo = halves(cols[source, c])
        split_c[c, :, :128] = hi
        split_c[c, :, 128:] = lo
        copies = {}

        def send(q, step, src, dst, link):
            copies[q, step] = remote(src, dst, f_send.at[f, c, q, step], f_recv.at[f, c, q, step], me.partner(link))
            copies[q, step].start()

        def multiply(q, carry):
            strip = rows_at(512 * q, 512)
            both = split_c[c]
            product = dot(m_hi[strip, :], both) + dot(m_lo[strip, :], both)
            part[c, strip, :] = product[:, :128] + product[:, 128:]
            for u in range(2):
                links = [STREAMS[2 * i + u][0] for i in range(4)]
                k1 = chosen(q, [me.bit(link) for link in links])
                there = [chosen(q, [me.partner(link)[i] for link in links]) for i in range(4)]
                remote(
                    part.at[c, rows_at(512 * q + 256 * u + 128 * (1 - k1), 128)], r1.at[f, c, 2 * q + u],
                    f_send.at[f, c, 2 * q + u, 0], f_recv.at[f, c, 2 * q + u, 0], tuple(there),
                ).start()
            return carry

        lax.fori_loop(0, 4, multiply, 0)
        where1, where2 = [], []
        for q, (l1, l2, l3, l4) in enumerate(STREAMS):
            k1, k2 = me.bit(l1), me.bit(l2)
            where1.append(256 * q + 128 * k1)
            where2.append(256 * q + 128 * k1 + 64 * k2)
            copies[q, 0] = remote(
                part.at[c, rows_at(256 * q + 128 * (1 - k1), 128)], r1.at[f, c, q],
                f_send.at[f, c, q, 0], f_recv.at[f, c, q, 0], me.partner(l1),
            )
        yield
        for q, (l1, l2, l3, l4) in enumerate(STREAMS):
            k2 = me.bit(l2)
            copies[q, 0].wait_recv()
            h1[c, q] = part[c, rows_at(where1[q], 128), :] + r1[f, c, q]
            send(q, 1, h1.at[c, q, rows_at(64 * (1 - k2), 64)], r2.at[f, c, q], l2)
        yield
        for q, (l1, l2, l3, l4) in enumerate(STREAMS):
            k2 = me.bit(l2)
            copies[q, 1].wait_recv()
            h2[c, q] = h1[c, q, rows_at(64 * k2, 64), :] + r2[f, c, q]
            if not last:
                send(q, 2, h2.at[c, q], r3.at[f, c, q], l3)
        if last:
            for copy in copies.values():
                copy.wait_send()
            return
        yield
        for q, (l1, l2, l3, l4) in enumerate(STREAMS):
            copies[q, 2].wait_recv()
            h3[c, q] = h2[c, q] + r3[f, c, q]
            send(q, 3, h3.at[c, q], r4.at[f, c, q], l4)
        yield
        for q, (l1, l2, l3, l4) in enumerate(STREAMS):
            copies[q, 3].wait_recv()
            total = h3[c, q] + r4[f, c, q]
            here = rows_at(where2[q], 64)
            if before is not None:
                total = 2.0 * total - rows[before, c, here, :]
            rows[target, c, here, :] = total
            send(q, 4, rows.at[target, c, here], rows.at[target, c, here], l2)
        yield
        for q, (l1, l2, l3, l4) in enumerate(STREAMS):
            copies[q, 4].wait_recv()
            here = rows_at(where1[q], 128)
            send(q, 5, rows.at[target, c, here], rows.at[target, c, here], l1)
        yield
        for q in range(8):
            copies[q, 5].wait_recv()
        for copy in copies.values():
            copy.wait_send()

    def backward(c, b, source, target, before):
        def split(i, carry):
            strip = rows_at(512 * i, 512)
            hi, lo = halves(rows[source, c, strip, :])
            split_r[c, strip, :128] = hi
            split_r[c, strip, 128:] = lo
            return carry

        lax.fori_loop(0, 4, split, 0)
        orders = ("xa", "xb"), ("xb", "xa")
        copies = {}

        def send(s, step, src, dst, link):
            copies[s, step] = remote(src, dst, b_send.at[b, c, s, step], b_recv.at[b, c, s, step], me.partner(link))
            copies[s, step].start()

        def multiply(s, carry):
            strip = rows_at(256 * s, 256)
            both = split_r[c]
            product = dot(t_hi[strip, :], both) + dot(t_lo[strip, :], both)
            tb[c, strip, :] = product[:, :128] + product[:, 128:]
            for u in range(2):
                strip = rows_at(256 * s + 128 * u, 128)
                remote(
                    tb.at[c, strip], rb1.at[b, c, strip],
                    b_send.at[b, c, 2 * s + u, 0], b_recv.at[b, c, 2 * s + u, 0], me.partner(orders[u][0]),
                ).start()
            return carry

        lax.fori_loop(0, 2, multiply, 0)
        for s in range(4):
            strip = pl.ds(128 * s, 128)
            copies[s, 0] = remote(
                tb.at[c, strip], rb1.at[b, c, strip],
                b_send.at[b, c, s, 0], b_recv.at[b, c, s, 0], me.partner(orders[s % 2][0]),
            )
        yield
        for s in range(4):
            strip = pl.ds(128 * s, 128)
            copies[s, 0].wait_recv()
            tb2[c, strip, :] = tb[c, strip, :] + rb1[b, c, strip, :]
            send(s, 1, tb2.at[c, strip], rb2.at[b, c, strip], orders[s % 2][1])
        yield
        for s in range(4):
            strip = pl.ds(128 * s, 128)
            copies[s, 1].wait_recv()
            total = tb2[c, strip, :] + rb2[b, c, strip, :]
            if before is not None:
                total = 2.0 * total - cols[before, c, strip, :]
            cols[target, c, strip, :] = total
        for copy in copies.values():
            copy.wait_send()

    done = set()

    def chain(c):
        yield from forward(c, 0, 0, 0, None)
        yield from backward(c, 0, 0, 1, 0)
        yield from forward(c, 1, 1, 1, 0)
        done.add(("y3", c))
        yield from backward(c, 1, 1, 2, None)
        yield from forward(c, 2, 2, 2, 1)
        yield from backward(c, 2, 2, 3, 2)
        done.add(("v3", c))
        yield from forward(c, 3, 3, None, None, last=True)
        mine = lanes_at(256 * me.core + 128 * c, 128)
        pending = []
        own_index = None
        for q, (l1, l2, l3, l4) in enumerate(STREAMS):
            k1, k2, k3, k4 = me.bit(l1), me.bit(l2), me.bit(l3), me.bit(l4)
            to_x, to_y, to_z = 2 * (q % 2) + k1, q // 2, me.x
            index = 2 * k3 + k4
            same = (to_x == me.x) & (to_y == me.y) & (to_z == me.z)
            own_index = jnp.where(same, 4 * k2 + index, -1 if own_index is None else own_index)
            copy = remote(
                h2.at[c, q], share.at[c, k2, index],
                p_send.at[c, q], p_recv.at[c, k2, index], me.device(x=to_x, y=to_y, z=to_z),
            )

            @pl.when(jnp.logical_not(same))
            def _():
                copy.start()

            @pl.when(same)
            def _():
                share[c, k2, index] = h2[c, q]

            pending.append((same, copy))
        yield
        for same, copy in pending:

            @pl.when(jnp.logical_not(same))
            def _():
                copy.wait_send()

        for k2 in range(2):
            for index in range(4):

                @pl.when(own_index != 4 * k2 + index)
                def _():
                    remote(
                        h2.at[c, 0], share.at[c, k2, index], p_send.at[c, 0], p_recv.at[c, k2, index], me.sibling()
                    ).wait_recv()

            pieces = [share[c, k2, index] for index in range(4)]
            full[2, pl.ds(64 * k2, 64), mine] = (pieces[0] + pieces[1]) + (pieces[2] + pieces[3])
        done.add(("z2", c))

    half = lanes_at(256 * me.core, 256)

    def needs(*marks):
        while not all(mark in done for mark in marks):
            yield "blocked"

    def swap_slab(k):
        copy = remote(full.at[k, :, half], full.at[k, :, half], s_send.at[k], s_recv.at[k], me.sibling())
        copy.start()
        yield
        copy.wait()

    def all_sum(n, target):
        def piece(s, k):
            return pl.ds(pl.multiple_of(SUM_START[s] + SUM_HALF[s] * k, 8), SUM_HALF[s])

        small = [pl.ds(0, SUM_HALF[s]) for s in range(6)]
        keep = [piece(s, me.bit(order[0])) for s, order in enumerate(SUM_LINKS)]
        away = [piece(s, 1 - me.bit(order[0])) for s, order in enumerate(SUM_LINKS)]
        copies = {}
        for s, order in enumerate(SUM_LINKS):
            for t in range(7):
                if t == 0:
                    src, dst = local.at[n, away[s]], got.at[n, 0, s, small[s]]
                elif t < 6:
                    src, dst = term.at[n % 2, t - 1, s, small[s]], got.at[n, t, s, small[s]]
                else:
                    src = dst = total.at[n, keep[s]]
                link = order[t % 6]
                copies[s, t] = remote(src, dst, a_send.at[n, s, t], a_recv.at[n, s, t], me.partner(link))
        copy = remote(total.at[n], target.at[:, half], x_send.at[n], x_recv.at[n], me.sibling())
        for s in range(6):
            copies[s, 0].start()
        yield
        for t in range(1, 6):
            for s in range(6):
                copies[s, t - 1].wait_recv()
                before = local[n, keep[s], :] if t == 1 else term[n % 2, t - 2, s, small[s], :]
                term[n % 2, t - 1, s, small[s], :] = before + got[n, t - 1, s, small[s], :]
                copies[s, t].start()
            yield
        for s in range(6):
            copies[s, 5].wait_recv()
            total[n, keep[s], :] = term[n % 2, 4, s, small[s], :] + got[n, 5, s, small[s], :]
            copies[s, 6].start()
        yield
        for s in range(6):
            copies[s, 6].wait_recv()
        copy.start()
        target[:, half] = total[n]
        for one in copies.values():
            one.wait_send()
        yield
        copy.wait()

    def keep_transposed(x):
        for i, one in enumerate(thirds(x[...].T)):
            turned[i] = one

    def transposed():
        return turned[0], turned[1], turned[2]

    def first_factor():
        yield from needs(("y3", 0), ("y3", 1))
        for c in range(2):
            full[0, :, lanes_at(256 * me.core + 128 * c, 128)] = rows[1, c, rows_at(block * 128, 128), :]
        yield from swap_slab(0)
        local[0] = precise_gram(thirds(full[0]), thirds(full[0, :, half])) / 8192
        yield from all_sum(0, inverse.at[0])
        for k in range(8):
            factor_block(inverse.at[0], jnp.int32(k), 128 * ((k + 1) // 2))
            yield
        lower_only(inverse.at[0])
        keep_transposed(inverse.at[0])
        done.add("first")

    def second_factor():
        yield from needs(("v3", 0), ("v3", 1))
        for c in range(2):
            full[1, :, lanes_at(256 * me.core + 128 * c, 128)] = cols[3, c, rows_at(me.x * 128, 128), :]
        yield from swap_slab(1)
        yield from needs("first")
        mapped[0] = precise(thirds(full[1]), transposed())
        local[1] = precise_gram(thirds(mapped[0]), thirds(mapped[0, :, half])) / 8192
        done.add("filtered")
        yield from all_sum(1, inverse.at[1])

    def cross_terms():
        yield from needs(("z2", 0), ("z2", 1), "filtered")
        yield from swap_slab(2)
        mapped[1] = precise(thirds(full[2]), transposed())
        local[2] = precise_gram(thirds(mapped[0]), thirds(mapped[1, :, half])) / 8192
        yield from all_sum(2, cross)

    crossing = cross_terms()
    live = [second_factor(), chain(0), chain(1), first_factor(), crossing]
    while len(live) > 1:
        for one in list(live):
            if next(one, "end") == "end":
                live.remove(one)

    def factor_and_cross(k, carry):
        factor_block(inverse.at[1], k)
        for i in range(8):

            @pl.when(k == i)
            def _():
                next(crossing, "end")

        return carry

    lax.fori_loop(0, 8, factor_and_cross, 0)
    for _ in crossing:
        pass
    lower_only(inverse.at[1])

    keep_transposed(inverse.at[1])
    mine = rows_at(64 * me.core, 64)
    basis = precise(thirds(mapped[0, mine, :]), transposed())
    basis_out[...] = basis
    for i, one in enumerate(thirds(cross[...])):
        parts[i] = one

    def solve_left(i, carry):
        strip = rows_at(256 * i, 256)
        cross[strip, :] = precise(thirds(inverse[1, strip, :]), (parts[0], parts[1], parts[2]))
        return carry

    lax.fori_loop(0, 2, solve_left, 0)

    def solve_right(i, carry):
        strip = rows_at(256 * i, 256)
        proj_out[strip, :] = precise(thirds(cross[strip, :]), transposed())
        return carry

    lax.fori_loop(0, 2, solve_right, 0)
    rest = mapped[1, mine, :] - precise(thirds(basis), thirds(cross[...]))
    resid_out[...] = precise(thirds(rest), transposed())


def chain_call(matrix, slab, interval):
    vm = pl.BlockSpec(memory_space=pltpu.VMEM)
    dma = pltpu.SemaphoreType.DMA
    slab_shape = jax.ShapeDtypeStruct((64, 512), F32)
    return pl.pallas_call(
        chain_kernel,
        out_shape=(slab_shape, jax.ShapeDtypeStruct((512, 512), F32), slab_shape),
        in_specs=[pl.BlockSpec(memory_space=pltpu.SMEM), vm, vm],
        out_specs=(vm, vm, vm),
        scratch_shapes=[
            pltpu.VMEM((1024, 512), F32),
            pltpu.VMEM((2048, 512), BF16),
            pltpu.VMEM((2048, 512), BF16),
            pltpu.VMEM((512, 2048), BF16),
            pltpu.VMEM((512, 2048), BF16),
            pltpu.VMEM((4, 2, 512, 128), F32),
            pltpu.VMEM((3, 2, 2048, 128), F32),
            pltpu.VMEM((2, 2048, 128), F32),
            pltpu.VMEM((2, 512, 256), BF16),
            pltpu.VMEM((2, 2048, 256), BF16),
            pltpu.VMEM((4, 2, 8, 128, 128), F32),
            pltpu.VMEM((2, 8, 128, 128), F32),
            pltpu.VMEM((4, 2, 8, 64, 128), F32),
            pltpu.VMEM((2, 8, 64, 128), F32),
            pltpu.VMEM((3, 2, 8, 64, 128), F32),
            pltpu.VMEM((2, 8, 64, 128), F32),
            pltpu.VMEM((3, 2, 8, 64, 128), F32),
            pltpu.VMEM((2, 2, 4, 64, 128), F32),
            pltpu.VMEM((2, 512, 128), F32),
            pltpu.VMEM((3, 2, 512, 128), F32),
            pltpu.VMEM((2, 512, 128), F32),
            pltpu.VMEM((3, 2, 512, 128), F32),
            pltpu.VMEM((3, 128, 512), F32),
            pltpu.VMEM((2, 128, 512), F32),
            pltpu.VMEM((3, 512, 256), F32),
            pltpu.VMEM((3, 512, 256), F32),
            pltpu.VMEM((2, 5, 6, 48, 256), F32),
            pltpu.VMEM((3, 6, 6, 48, 256), F32),
            pltpu.VMEM((2, 512, 512), F32),
            pltpu.VMEM((512, 512), F32),
            pltpu.VMEM((3, 512, 512), BF16),
            pltpu.VMEM((3, 512, 512), BF16),
            dma((4, 2, 8, 6)),
            dma((4, 2, 8, 6)),
            dma((3, 2, 4, 2)),
            dma((3, 2, 4, 2)),
            dma((8, 2)),
            dma((8, 2)),
            dma,
            dma,
            dma((2, 8)),
            dma((2, 2, 4)),
            dma((3,)),
            dma((3,)),
            dma((3, 6, 7)),
            dma((3, 6, 7)),
            dma((3,)),
            dma((3,)),
        ],
        compiler_params=pltpu.CompilerParams(has_side_effects=True, collective_id=0, vmem_limit_bytes=VMEM_LIMIT),
    )(interval, matrix, slab)


def shards(matrix, start_vectors, interval):
    return chain_call(matrix, start_vectors, interval)


def solution(mesh):
    torus = Mesh(mesh.devices.reshape(4, 2, 4, 4), ("row_0", "row_1", "col_0", "col_1"))
    placed = (P(ROW, COL), P(COL_ROW, None), P())
    return jax.shard_map(
        shards,
        mesh=torus,
        in_specs=placed,
        out_specs=(P(COL_ROW, None), P(), P(COL_ROW, None)),
        check_vma=False,
    )
```
